32 devices in a mesh: turn: 4 (over y, core), blk: 4 (over z), strip: 2 (over x).
Axes of the slice: x: 2, y: 2, z: 4, core: 2. Of those that a mesh axis runs over, the one named last changes fastest.
Arguments:
- echoes: bfloat16 [2, 256, 32768], P(None, 'blk', ('turn', 'strip')), may hold values from -6 to 6
- filters: bfloat16 [2, 8, 32768], P(None, 'blk'), may hold values from -6 to 6
- slab_index: int32 [256], P(('blk', 'turn')), may hold values from 0 to 7
- shifts: int32 [256], P(('blk', 'turn')), may hold values from 0 to 32767
Outputs:
- focused: float32 [2, 256, 32768], P(None, ('blk', 'turn'), 'strip')
The draws below stay inside these ranges and needn't reach their ends.
All inputs are finite; a program needn't handle non-finite values.
Results may differ from the reference program's by a relative error of at most 0.0003.
Values may be sent and summed in bfloat16 or wider, within the bound.
A program may use at most 128 MiB of HBM per device.

```python
import jax
import jax.numpy as jnp
from jax import lax

NA = 32768
NR = 256
NS = 8


def plant(entries, stream_key, smallest, largest):
    dims = entries.shape
    place = [jax.random.randint(jax.random.fold_in(stream_key, axis), (), 0, dims[axis]) for axis in range(len(dims))]
    entries = entries.at[tuple(place)].set(smallest)
    longest = dims.index(max(dims))
    place[longest] = (place[longest] + 1) % dims[longest]
    return entries.at[tuple(place)].set(largest)


def block_scale(own_key, extent, split, smallest, high):
    loudness, own = 1.0, jax.random.fold_in(own_key, 6)
    for dim, blocks in split:
        steps = jnp.exp(jax.random.uniform(jax.random.fold_in(own, dim), (blocks,), jnp.float32, smallest / len(split), high / len(split)))
        loudness = loudness * jnp.repeat(steps, extent[dim] // blocks).reshape([-1 if axis == dim else 1 for axis in range(len(extent))])
    return loudness


def scatter_about(rng, shape, scale, limit, split=(), kind=jnp.bfloat16):
    values = jax.random.normal(rng, shape, jnp.float32) * scale
    if len(split) > 0:
        values = block_scale(rng, shape, split, -0.22, 0.18) * values
    return jnp.clip(values, min=-limit, max=limit).astype(kind)


def setup_inputs(seed: int = 0) -> dict:
    key_of = jax.random.split(jax.random.key(seed), 5)
    echoes = scatter_about(key_of[0], (2, NR, NA), 1.0, 6.0, ((1, 4), (2, 8)))
    filters = scatter_about(key_of[1], (2, NS, NA), 1.0, 6.0, ((1, 4),))
    slab_index = plant(jax.random.randint(key_of[2], (NR,), 0, NS), jax.random.fold_in(key_of[2], 1), 0, NS - 1).astype(jnp.int32)
    shifts = plant(jax.random.randint(key_of[3], (NR,), 0, NA), jax.random.fold_in(key_of[3], 1), 0, NA - 1).astype(jnp.int32)
    return dict(echoes=echoes, filters=filters, slab_index=slab_index, shifts=shifts)


def reference(echoes, filters, slab_index, shifts):
    signal = lax.complex(echoes[0].astype(jnp.float32), echoes[1].astype(jnp.float32))
    spectrum = jnp.fft.fft(signal, axis=1)
    chosen = lax.complex(filters[0][slab_index].astype(jnp.float32), filters[1][slab_index].astype(jnp.float32))
    image = jnp.fft.ifft(spectrum * chosen, axis=1)
    positions = (jnp.arange(NA, dtype=jnp.int32)[None, :] - shifts[:, None].astype(jnp.int32)) % NA
    rolled = jnp.take_along_axis(image, positions, axis=1)
    return jnp.stack([jnp.real(rolled), jnp.imag(rolled)]).astype(jnp.float32)
```

```python
import functools
import math

import jax
import jax.numpy as jnp
import numpy as np
from jax import lax
from jax.experimental import pallas as pl
from jax.experimental.pallas import tpu as pltpu
from jax.sharding import PartitionSpec as P

LANES = 128
PAIR = 2
MESH = pl.DeviceIdType.MESH
f32, bf16 = jnp.float32, jnp.bfloat16


def split_np(table):
    high = table.astype(jnp.bfloat16)
    low = (table - high.astype(np.float64)).astype(jnp.bfloat16)
    return high, low


def make_tables(length, sources, strips):
    half = LANES
    outer = length // (2 * half)
    local = outer // sources
    a_ids, c_ids = np.arange(outer), np.arange(outer)
    b_ids = np.arange(half)
    tau = np.exp(-2j * np.pi * half * c_ids / length)
    first = np.exp(-2j * np.pi * ((c_ids[:, None] * a_ids[None, :]) % outer) / outer)
    stage_one = []
    for mat in (first, tau[:, None] * first):
        grouped = mat.reshape(outer, sources, 1, local)
        top = np.concatenate([grouped.real, -grouped.imag], 2).reshape(outer, 2 * outer)
        bottom = np.concatenate([grouped.imag, grouped.real], 2).reshape(outer, 2 * outer)
        stage_one.append(np.concatenate(split_np(np.concatenate([top, bottom], 0)), 0))
    stage_one = np.stack(stage_one)
    base = np.exp(-2j * np.pi * ((b_ids[:, None] * b_ids[None, :]) % half) / half)

    def right(mat):
        whole = np.concatenate(
            [np.concatenate([mat.real, mat.imag], 1), np.concatenate([-mat.imag, mat.real], 1)], 0
        )
        high, low = split_np(whole)
        return np.concatenate([high, low, high], 0)

    stage_two = np.stack([right(base), right(base.conj())])
    twist = np.exp(-2j * np.pi * ((c_ids[:, None] * b_ids[None, :]) % length) / length)
    omega = np.exp(-2j * np.pi * b_ids / (2 * half))
    turned = twist * omega[None, :]
    twists = np.stack([twist.real, twist.imag, turned.real, turned.imag]).astype(np.float32)
    rows = outer // strips
    last = []
    for strip in range(strips):
        picked = np.arange(strip * rows, (strip + 1) * rows)
        back = np.exp(2j * np.pi * ((picked[:, None] * c_ids[None, :]) % outer) / outer) / length
        per_half = []
        for mat in (back, back * tau.conj()[None, :]):
            whole = np.concatenate(
                [np.concatenate([mat.real, -mat.imag], 1), np.concatenate([mat.imag, mat.real], 1)], 0
            )
            per_half.append(np.concatenate(split_np(whole), 0))
        last.append(np.stack(per_half))
    return stage_one, stage_two, twists, np.stack(last)


def cosine_sine(phase, length):
    quarter = length // 4
    wrapped = phase & (length - 1)
    quadrant = (wrapped + quarter // 2) // quarter if quarter & (quarter - 1) else (
        wrapped + quarter // 2
    ) >> (quarter.bit_length() - 1)
    angle = (wrapped - quadrant * quarter).astype(f32) * (2.0 * math.pi / length)
    square = angle * angle
    sine = angle * (
        1.0 + square * (-1.0 / 6 + square * (1.0 / 120 + square * (-1.0 / 5040 + square * (1.0 / 362880))))
    )
    cosine = 1.0 + square * (
        -0.5
        + square * (1.0 / 24 + square * (-1.0 / 720 + square * (1.0 / 40320 - square * (1.0 / 3628800))))
    )
    odd = (quadrant & 1) == 1
    out_cos = jnp.where(odd, sine, cosine)
    out_sin = jnp.where(odd, cosine, sine)
    quad = quadrant & 3
    out_cos = jnp.where((quad == 1) | (quad == 2), -out_cos, out_cos)
    out_sin = jnp.where(quad >= 2, -out_sin, out_sin)
    return out_cos, out_sin


def cmul(ar, ai, br, bi):
    return ar * br - ai * bi, ar * bi + ai * br


def split(values):
    high = values.astype(bf16)
    return high, (values - high.astype(f32)).astype(bf16)


def dot(left, right):
    return jnp.dot(left, right, preferred_element_type=f32)


def body(
    turns, blks, strips, length,
    shifts_ref, slabs_ref, ech_ref, filt_ref, one_hbm, two_hbm, twist_hbm, last_hbm,
    out_ref,
    recv, filt_all, inv_twist, ramp, spec, one_ref, two_ref, twist_ref, last_ref, ech_raw, filt_raw, staged, outbox,
    send_sem, recv_sem, fsend, frecv, gsend, grecv, load_sem,
):
    turn, blk, strip = lax.axis_index("turn"), lax.axis_index("blk"), lax.axis_index("strip")
    pairs = recv.shape[0]
    row_count = pairs * PAIR
    slab_local = filt_ref.shape[1] * LANES // length
    core = lax.rem(turn, 2)
    partner = turn + 1 - 2 * core
    peers = [(dt, ds) for dt in range(turns) for ds in range(strips) if (dt, ds) != (0, 0)]

    def peer(dt, ds):
        return (lax.rem(turn + dt, turns), blk, lax.rem(strip + ds, strips))

    me = turn * strips + strip
    twist_load = pltpu.make_async_copy(twist_hbm, twist_ref, load_sem.at[0])
    one_load = pltpu.make_async_copy(one_hbm, one_ref, load_sem.at[1])
    two_load = pltpu.make_async_copy(two_hbm, two_ref, load_sem.at[2])
    last_load = pltpu.make_async_copy(last_hbm.at[strip], last_ref, load_sem.at[3])
    echo_load = pltpu.make_async_copy(ech_ref, ech_raw, load_sem.at[4])
    filter_load = pltpu.make_async_copy(filt_ref, filt_raw, load_sem.at[5])
    echo_load.start()
    filter_load.start()

    barrier = pltpu.get_barrier_semaphore()
    for dt, ds in peers:
        pl.semaphore_signal(barrier, inc=1, device_id=peer(dt, ds), device_id_type=MESH)
    for dz in range(1, blks):
        pl.semaphore_signal(
            barrier, inc=1, device_id=(turn, lax.rem(blk + dz, blks), strip), device_id_type=MESH
        )
    twist_load.start()
    one_load.start()
    two_load.start()
    last_load.start()
    pl.semaphore_wait(barrier, len(peers) + blks - 1)

    def echo_copy(step, dt, ds):
        to = peer(dt, ds)
        return pltpu.make_async_remote_copy(
            src_ref=outbox.at[to[0], step],
            dst_ref=recv.at[step, me],
            send_sem=send_sem.at[step, dt * strips + ds],
            recv_sem=recv_sem.at[step, dt * strips + ds],
            device_id=to,
            device_id_type=MESH,
        )

    def filter_copy(dz):
        return pltpu.make_async_remote_copy(
            src_ref=filt_all.at[pl.ds(blk * slab_local, slab_local), core],
            dst_ref=filt_all.at[pl.ds(blk * slab_local, slab_local), core],
            send_sem=fsend.at[dz],
            recv_sem=frecv.at[dz],
            device_id=(turn, lax.rem(blk + dz, blks), strip),
            device_id_type=MESH,
        )

    def relay_copy(dz):
        origin = lax.rem(blk + blks - dz, blks)
        place = filt_all.at[pl.ds(origin * slab_local, slab_local), core]
        return pltpu.make_async_remote_copy(
            src_ref=place,
            dst_ref=place,
            send_sem=gsend.at[dz],
            recv_sem=grecv.at[dz],
            device_id=(partner, blk, strip),
            device_id_type=MESH,
        )

    half = LANES
    outer = length // (2 * half)
    local = ech_raw.shape[2] // 2
    groups = row_count // 8
    per_group = 8 // PAIR

    def arrange(group):
        def fill(to, carry):
            for part in range(2):
                values = ech_raw[part, to * groups + group].astype(f32)
                staged[part] = values.reshape(2 * local * 8, half)
            for part in range(2):
                for row in range(8):
                    for side in range(2):
                        value = staged[part, pl.ds(side * 8 + row, local, stride=16), :]
                        outbox[
                            to, group * per_group + row // PAIR, part, row % PAIR, :,
                            side * half : (side + 1) * half,
                        ] = value.astype(bf16)
            return carry

        lax.fori_loop(0, turns, fill, 0)
        first, end = group * per_group, (group + 1) * per_group

        def start_step(step, carry):
            for dt, ds in peers:
                echo_copy(step, dt, ds).start()
            return carry

        lax.fori_loop(first, end, start_step, 0)

        def keep(step, carry):
            recv[step, me] = outbox[turn, step]
            return carry

        lax.fori_loop(first, end, keep, 0)

    echo_load.wait()
    arrange(0)
    filter_load.wait()
    bins = filt_raw.shape[1]
    bin_ids = lax.broadcasted_iota(jnp.int32, (bins, half), 0)
    d_ids = lax.broadcasted_iota(jnp.int32, (bins, half), 1)
    for s in range(slab_local):
        for e in range(2):
            picker = (bin_ids == (d_ids * 2 + e) * slab_local + s).astype(f32).astype(bf16)
            for part in range(2):
                got = lax.dot_general(
                    filt_raw[part], picker, (((0,), (0,)), ((), ())), preferred_element_type=f32
                )
                filt_all[blk * slab_local + s, part, e] = got.astype(bf16)
    for dz in range(1, blks):
        filter_copy(dz).start()
    for group in range(1, groups):
        arrange(group)

    c_ids = lax.broadcasted_iota(jnp.int32, (outer, half), 0)
    lane_ids = lax.broadcasted_iota(jnp.int32, (8, 2 * half), 1)
    k_ids = jnp.where(lane_ids >= half, (lane_ids - half) * (2 * outer) + outer, lane_ids * (2 * outer))

    def prepare(row, carry):
        shift = shifts_ref[row]
        vr, vi = cosine_sine(c_ids * shift, length)
        vi = -vi
        for part in range(2):
            tr, ti = twist_ref[2 * part], -twist_ref[2 * part + 1]
            rr, ri = cmul(tr, ti, vr, vi)
            inv_twist[row, 2 * part] = rr
            inv_twist[row, 2 * part + 1] = ri
        ur, ui = cosine_sine(k_ids * shift, length)
        ramp[row, 0] = ur
        ramp[row, 1] = -ui
        return carry

    twist_load.wait()
    lax.fori_loop(0, row_count, prepare, 0)
    one_load.wait()
    two_load.wait()

    def lefts(blocks):
        highs, lows = [], []
        for re, im in blocks:
            high, low = split(jnp.concatenate([re, im], 1))
            highs.append(high)
            lows.append(low)
        high, low = jnp.concatenate(highs, 0), jnp.concatenate(lows, 0)
        return jnp.concatenate([high, high, low], 1)

    def forward(step, carry):
        for dt, ds in peers:
            echo_copy(step, dt, ds).wait_recv()
        rows = [recv[step, :, :, i].reshape(2 * outer, 2 * half) for i in range(PAIR)]
        parts = []
        for side in range(2):
            lanes = slice(side * half, (side + 1) * half)
            res = dot(one_ref[side], jnp.concatenate([r[:, lanes] for r in rows], 1))
            parts.append(res[: 2 * outer] + res[2 * outer :])
        total, differ = parts[0] + parts[1], parts[0] - parts[1]
        blocks = []
        for e, value in enumerate((total, differ)):
            tr, ti = twist_ref[2 * e], twist_ref[2 * e + 1]
            for i in range(PAIR):
                lanes = slice(i * half, (i + 1) * half)
                blocks.append(cmul(value[:outer, lanes], value[outer:, lanes], tr, ti))
        spec[step] = dot(lefts(blocks), two_ref[0])
        return carry

    def inverse(step, carry):
        blocks = []
        for e in range(2):
            lanes = slice(e * half, (e + 1) * half)
            for i in range(PAIR):
                row = step * PAIR + i
                picked = filt_all[slabs_ref[row], :, e].astype(f32)
                ur, ui = ramp[row, 0][:1, lanes], ramp[row, 1][:1, lanes]
                gr, gi = cmul(picked[0], picked[1], ur, ui)
                base = (e * PAIR + i) * outer
                z = spec[step, base : base + outer]
                blocks.append(cmul(z[:, :half], z[:, half:], gr, gi))
        back = dot(lefts(blocks), two_ref[1])
        lows, highs = [], []
        for i in range(PAIR):
            row = step * PAIR + i
            got = []
            for e in range(2):
                base = (e * PAIR + i) * outer
                u = back[base : base + outer]
                got.append(
                    cmul(u[:, :half], u[:, half:], inv_twist[row, 2 * e], inv_twist[row, 2 * e + 1])
                )
            lows.append(jnp.concatenate([got[0][0] + got[1][0], got[0][1] + got[1][1]], 0))
            highs.append(jnp.concatenate([got[0][0] - got[1][0], got[0][1] - got[1][1]], 0))
        rows = outer // strips
        for side, value in enumerate((lows, highs)):
            high, low = split(jnp.concatenate(value, 1))
            left = last_ref[side]
            res = dot(left, high)
            res = res[: 2 * rows] + res[2 * rows :] + dot(left[: 2 * rows], low)
            for i in range(PAIR):
                place = lax.rem(step, 8 // PAIR) * PAIR + i + 8 * side
                for part in range(2):
                    out_ref[part, step // (8 // PAIR), pl.ds(place, rows, stride=16), :] = res[
                        part * rows : (part + 1) * rows, i * half : (i + 1) * half
                    ]
        return carry

    def both(step, carry):
        forward(step, 0)
        inverse(step, 0)
        return carry

    early = pairs // 2
    lax.fori_loop(0, early, forward, 0)
    for dz in range(1, blks):
        filter_copy(dz).wait_recv()
        relay_copy(dz).start()
    for dz in range(1, blks):
        relay_copy(dz).wait_recv()
    last_load.wait()
    lax.fori_loop(0, early, inverse, 0)
    lax.fori_loop(early, pairs, both, 0)

    def end_step(step, carry):
        for dt, ds in peers:
            echo_copy(step, dt, ds).wait_send()
        return carry

    lax.fori_loop(0, pairs, end_step, 0)
    for dz in range(1, blks):
        filter_copy(dz).wait_send()
        relay_copy(dz).wait_send()


def per_device(turns, blks, strips, echoes, filters, slab_index, shifts):
    sources = turns * strips
    length = filters.shape[2]
    half = LANES
    outer = length // (2 * half)
    local = outer // sources
    row_count = slab_index.shape[0]
    slab_local = filters.shape[1]
    pairs = row_count // PAIR
    shaped = echoes.reshape(2, -1, 8, 2 * local, half).transpose(0, 1, 3, 2, 4)
    response = filters.reshape(2, slab_local, 2 * outer, half).transpose(0, 2, 1, 3)
    response = response.reshape(2, -1, half)
    tables = [jnp.asarray(t) for t in make_tables(length, sources, strips)]
    hbm, smem = pl.BlockSpec(memory_space=pltpu.HBM), pl.BlockSpec(memory_space=pltpu.SMEM)
    rows = outer // strips
    image = pl.pallas_call(
        functools.partial(body, turns, blks, strips, length),
        out_shape=pltpu.VMEM((2, row_count // 8, rows * 16, half), f32),
        in_specs=[smem, smem] + [hbm] * 6,
        out_specs=pl.BlockSpec(memory_space=pltpu.VMEM),
        scratch_shapes=[
            pltpu.VMEM((pairs, sources, 2, PAIR, local, 2 * half), bf16),
            pltpu.VMEM((slab_local * blks, 2, 2, outer, half), bf16),
            pltpu.VMEM((row_count, 4, outer, half), f32),
            pltpu.VMEM((row_count, 2, 8, 2 * half), f32),
            pltpu.VMEM((pairs, 2 * PAIR * outer, 2 * half), f32),
            pltpu.VMEM(tables[0].shape, bf16),
            pltpu.VMEM(tables[1].shape, bf16),
            pltpu.VMEM(tables[2].shape, f32),
            pltpu.VMEM(tables[3].shape[1:], bf16),
            pltpu.VMEM(shaped.shape, bf16),
            pltpu.VMEM(response.shape, bf16),
            pltpu.VMEM((2, 16 * local, half), f32),
            pltpu.VMEM((turns, pairs, 2, PAIR, local, 2 * half), bf16),
            pltpu.SemaphoreType.DMA((pairs, sources)),
            pltpu.SemaphoreType.DMA((pairs, sources)),
            pltpu.SemaphoreType.DMA((blks,)),
            pltpu.SemaphoreType.DMA((blks,)),
            pltpu.SemaphoreType.DMA((blks,)),
            pltpu.SemaphoreType.DMA((blks,)),
            pltpu.SemaphoreType.DMA((6,)),
        ],
        compiler_params=pltpu.CompilerParams(
            collective_id=0, has_side_effects=True, vmem_limit_bytes=56 * 1024 * 1024
        ),
    )(shifts, slab_index, shaped, response, *tables)
    image = image.reshape(2, row_count // 8, rows * 2, 8, half).transpose(0, 1, 3, 2, 4)
    return image.reshape(2, row_count, rows * 2 * half)


def solution(mesh):
    in_specs = (
        P(None, "blk", ("turn", "strip")),
        P(None, "blk", None),
        P(("blk", "turn")),
        P(("blk", "turn")),
    )
    out_specs = P(None, ("blk", "turn"), "strip")
    local = functools.partial(
        per_device, mesh.shape["turn"], mesh.shape["blk"], mesh.shape["strip"]
    )
    return jax.shard_map(local, mesh=mesh, in_specs=in_specs, out_specs=out_specs, check_vma=False)
```

```python
import functools
import math

import jax
import jax.numpy as jnp
import numpy as np
from jax import lax
from jax.experimental import pallas as pl
from jax.experimental.pallas import tpu as pltpu
from jax.sharding import PartitionSpec as P

LANES = 128
PAIR = 2
MESH = pl.DeviceIdType.MESH
f32, bf16 = jnp.float32, jnp.bfloat16


def split_np(table):
    high = table.astype(jnp.bfloat16)
    low = (table - high.astype(np.float64)).astype(jnp.bfloat16)
    return high, low


def make_tables(length, sources, strips):
    half = LANES
    outer = length // (2 * half)
    local = outer // sources
    a_ids, c_ids = np.arange(outer), np.arange(outer)
    b_ids = np.arange(half)
    tau = np.exp(-2j * np.pi * half * c_ids / length)
    first = np.exp(-2j * np.pi * ((c_ids[:, None] * a_ids[None, :]) % outer) / outer)
    stage_one = []
    for mat in (first, tau[:, None] * first):
        grouped = mat.reshape(outer, sources, 1, local)
        top = np.concatenate([grouped.real, -grouped.imag], 2).reshape(outer, 2 * outer)
        bottom = np.concatenate([grouped.imag, grouped.real], 2).reshape(outer, 2 * outer)
        stage_one.append(np.concatenate(split_np(np.concatenate([top, bottom], 0)), 0))
    stage_one = np.stack(stage_one)
    base = np.exp(-2j * np.pi * ((b_ids[:, None] * b_ids[None, :]) % half) / half)

    def right(mat):
        whole = np.concatenate(
            [np.concatenate([mat.real, mat.imag], 1), np.concatenate([-mat.imag, mat.real], 1)], 0
        )
        high, low = split_np(whole)
        return np.concatenate([high, low, high], 0)

    stage_two = np.stack([right(base), right(base.conj())])
    twist = np.exp(-2j * np.pi * ((c_ids[:, None] * b_ids[None, :]) % length) / length)
    omega = np.exp(-2j * np.pi * b_ids / (2 * half))
    turned = twist * omega[None, :]
    twists = np.stack([twist.real, twist.imag, turned.real, turned.imag]).astype(np.float32)
    rows = outer // strips
    last = []
    for strip in range(strips):
        picked = np.arange(strip * rows, (strip + 1) * rows)
        back = np.exp(2j * np.pi * ((picked[:, None] * c_ids[None, :]) % outer) / outer) / length
        per_half = []
        for mat in (back, back * tau.conj()[None, :]):
            whole = np.concatenate(
                [np.concatenate([mat.real, -mat.imag], 1), np.concatenate([mat.imag, mat.real], 1)], 0
            )
            per_half.append(np.concatenate(split_np(whole), 0))
        last.append(np.stack(per_half))
    return stage_one, stage_two, twists, np.stack(last)


def cosine_sine(phase, length):
    quarter = length // 4
    wrapped = phase & (length - 1)
    quadrant = (wrapped + quarter // 2) // quarter if quarter & (quarter - 1) else (
        wrapped + quarter // 2
    ) >> (quarter.bit_length() - 1)
    angle = (wrapped - quadrant * quarter).astype(f32) * (2.0 * math.pi / length)
    square = angle * angle
    sine = angle * (
        1.0 + square * (-1.0 / 6 + square * (1.0 / 120 + square * (-1.0 / 5040 + square * (1.0 / 362880))))
    )
    cosine = 1.0 + square * (
        -0.5
        + square * (1.0 / 24 + square * (-1.0 / 720 + square * (1.0 / 40320 - square * (1.0 / 3628800))))
    )
    odd = (quadrant & 1) == 1
    out_cos = jnp.where(odd, sine, cosine)
    out_sin = jnp.where(odd, cosine, sine)
    quad = quadrant & 3
    out_cos = jnp.where((quad == 1) | (quad == 2), -out_cos, out_cos)
    out_sin = jnp.where(quad >= 2, -out_sin, out_sin)
    return out_cos, out_sin


def cmul(ar, ai, br, bi):
    return ar * br - ai * bi, ar * bi + ai * br


def split(values):
    high = values.astype(bf16)
    return high, (values - high.astype(f32)).astype(bf16)


def dot(left, right):
    return jnp.dot(left, right, preferred_element_type=f32)


def body(
    turns, blks, strips, length,
    shifts_ref, slabs_ref, ech_ref, filt_ref, one_hbm, two_hbm, twist_hbm, last_hbm,
    out_ref,
    recv, filt_all, inv_twist, ramp, spec, one_ref, two_ref, twist_ref, last_ref, ech_raw, filt_raw, staged, outbox,
    send_sem, recv_sem, fsend, frecv, gsend, grecv, load_sem,
):
    turn, blk, strip = lax.axis_index("turn"), lax.axis_index("blk"), lax.axis_index("strip")
    pairs = recv.shape[0]
    row_count = pairs * PAIR
    slab_local = filt_ref.shape[1] * LANES // length
    core = lax.rem(turn, 2)
    partner = turn + 1 - 2 * core
    peers = [(dt, ds) for dt in range(turns) for ds in range(strips) if (dt, ds) != (0, 0)]

    def peer(dt, ds):
        return (lax.rem(turn + dt, turns), blk, lax.rem(strip + ds, strips))

    me = turn * strips + strip
    twist_load = pltpu.make_async_copy(twist_hbm, twist_ref, load_sem.at[0])
    one_load = pltpu.make_async_copy(one_hbm, one_ref, load_sem.at[1])
    two_load = pltpu.make_async_copy(two_hbm, two_ref, load_sem.at[2])
    last_load = pltpu.make_async_copy(last_hbm.at[strip], last_ref, load_sem.at[3])
    echo_load = pltpu.make_async_copy(ech_ref, ech_raw, load_sem.at[4])
    filter_load = pltpu.make_async_copy(filt_ref, filt_raw, load_sem.at[5])
    echo_load.start()
    filter_load.start()

    barrier = pltpu.get_barrier_semaphore()
    for dt, ds in peers:
        pl.semaphore_signal(barrier, inc=1, device_id=peer(dt, ds), device_id_type=MESH)
    twist_load.start()
    one_load.start()
    two_load.start()
    last_load.start()

    def signal_blk(to):
        pl.semaphore_signal(barrier, inc=1, device_id=(turn, to, strip), device_id_type=MESH)

    def echo_copy(step, dt, ds):
        to = peer(dt, ds)
        return pltpu.make_async_remote_copy(
            src_ref=outbox.at[to[0], step],
            dst_ref=recv.at[step, me],
            send_sem=send_sem.at[step, dt * strips + ds],
            recv_sem=recv_sem.at[step, dt * strips + ds],
            device_id=to,
            device_id_type=MESH,
        )

    def filter_copy(dz):
        return pltpu.make_async_remote_copy(
            src_ref=filt_all.at[pl.ds(blk * slab_local, slab_local), core],
            dst_ref=filt_all.at[pl.ds(blk * slab_local, slab_local), core],
            send_sem=fsend.at[dz],
            recv_sem=frecv.at[dz],
            device_id=(turn, lax.rem(blk + dz, blks), strip),
            device_id_type=MESH,
        )

    def relay_copy(dz):
        origin = lax.rem(blk + blks - dz, blks)
        place = filt_all.at[pl.ds(origin * slab_local, slab_local), core]
        return pltpu.make_async_remote_copy(
            src_ref=place,
            dst_ref=place,
            send_sem=gsend.at[dz],
            recv_sem=grecv.at[dz],
            device_id=(partner, blk, strip),
            device_id_type=MESH,
        )

    half = LANES
    outer = length // (2 * half)
    local = ech_raw.shape[2] // 2
    groups = row_count // 8
    per_group = 8 // PAIR

    def arrange(group):
        def fill(to, carry):
            for part in range(2):
                values = ech_raw[part, to * groups + group].astype(f32)
                staged[part] = values.reshape(2 * local * 8, half)
            for part in range(2):
                for row in range(8):
                    for side in range(2):
                        value = staged[part, pl.ds(side * 8 + row, local, stride=16), :]
                        outbox[
                            to, group * per_group + row // PAIR, part, row % PAIR, :,
                            side * half : (side + 1) * half,
                        ] = value.astype(bf16)
            return carry

        lax.fori_loop(0, turns, fill, 0)

    def send(group):
        first, end = group * per_group, (group + 1) * per_group

        def start_step(step, carry):
            for dt, ds in peers:
                echo_copy(step, dt, ds).start()
            return carry

        lax.fori_loop(first, end, start_step, 0)

        def keep(step, carry):
            recv[step, me] = outbox[turn, step]
            return carry

        lax.fori_loop(first, end, keep, 0)

    echo_load.wait()
    arrange(0)
    pl.semaphore_wait(barrier, len(peers) + jnp.where(blk > 0, 1, 0))
    send(0)

    @pl.when(blk < blks - 1)
    def _():
        signal_blk(blk + 1)

    @pl.when(blk == blks - 1)
    def _():
        signal_blk(blk - 1)

    for group in range(1, groups):
        arrange(group)
        send(group)
    filter_load.wait()
    bins = filt_raw.shape[1]
    bin_ids = lax.broadcasted_iota(jnp.int32, (bins, half), 0)
    d_ids = lax.broadcasted_iota(jnp.int32, (bins, half), 1)
    for s in range(slab_local):
        for e in range(2):
            picker = (bin_ids == (d_ids * 2 + e) * slab_local + s).astype(f32).astype(bf16)
            for part in range(2):
                got = lax.dot_general(
                    filt_raw[part], picker, (((0,), (0,)), ((), ())), preferred_element_type=f32
                )
                filt_all[blk * slab_local + s, part, e] = got.astype(bf16)
    for dz in range(1, blks):

        @pl.when(blk + dz >= blks)
        def _(dz=dz):
            filter_copy(dz).start()

    c_ids = lax.broadcasted_iota(jnp.int32, (outer, half), 0)
    lane_ids = lax.broadcasted_iota(jnp.int32, (8, 2 * half), 1)
    k_ids = jnp.where(lane_ids >= half, (lane_ids - half) * (2 * outer) + outer, lane_ids * (2 * outer))

    def prepare(row, carry):
        shift = shifts_ref[row]
        vr, vi = cosine_sine(c_ids * shift, length)
        vi = -vi
        for part in range(2):
            tr, ti = twist_ref[2 * part], -twist_ref[2 * part + 1]
            rr, ri = cmul(tr, ti, vr, vi)
            inv_twist[row, 2 * part] = rr
            inv_twist[row, 2 * part + 1] = ri
        ur, ui = cosine_sine(k_ids * shift, length)
        ramp[row, 0] = ur
        ramp[row, 1] = -ui
        return carry

    @pl.when(blk < blks - 1)
    def _():
        pl.semaphore_wait(barrier, 1)

        @pl.when(blk > 0)
        def _():
            signal_blk(blk - 1)

        for dz in range(1, blks):

            @pl.when(blk + dz < blks)
            def _(dz=dz):
                filter_copy(dz).start()

    twist_load.wait()
    lax.fori_loop(0, row_count, prepare, 0)

    one_load.wait()
    two_load.wait()

    def lefts(blocks):
        highs, lows = [], []
        for re, im in blocks:
            high, low = split(jnp.concatenate([re, im], 1))
            highs.append(high)
            lows.append(low)
        high, low = jnp.concatenate(highs, 0), jnp.concatenate(lows, 0)
        return jnp.concatenate([high, high, low], 1)

    def forward(step, carry):
        for dt, ds in peers:
            echo_copy(step, dt, ds).wait_recv()
        rows = [recv[step, :, :, i].reshape(2 * outer, 2 * half) for i in range(PAIR)]
        parts = []
        for side in range(2):
            lanes = slice(side * half, (side + 1) * half)
            res = dot(one_ref[side], jnp.concatenate([r[:, lanes] for r in rows], 1))
            parts.append(res[: 2 * outer] + res[2 * outer :])
        total, differ = parts[0] + parts[1], parts[0] - parts[1]
        blocks = []
        for e, value in enumerate((total, differ)):
            tr, ti = twist_ref[2 * e], twist_ref[2 * e + 1]
            for i in range(PAIR):
                lanes = slice(i * half, (i + 1) * half)
                blocks.append(cmul(value[:outer, lanes], value[outer:, lanes], tr, ti))
        spec[step] = dot(lefts(blocks), two_ref[0])
        return carry

    def inverse(step, carry):
        blocks = []
        for e in range(2):
            lanes = slice(e * half, (e + 1) * half)
            for i in range(PAIR):
                row = step * PAIR + i
                picked = filt_all[slabs_ref[row], :, e].astype(f32)
                ur, ui = ramp[row, 0][:1, lanes], ramp[row, 1][:1, lanes]
                gr, gi = cmul(picked[0], picked[1], ur, ui)
                base = (e * PAIR + i) * outer
                z = spec[step, base : base + outer]
                blocks.append(cmul(z[:, :half], z[:, half:], gr, gi))
        back = dot(lefts(blocks), two_ref[1])
        lows, highs = [], []
        for i in range(PAIR):
            row = step * PAIR + i
            got = []
            for e in range(2):
                base = (e * PAIR + i) * outer
                u = back[base : base + outer]
                got.append(
                    cmul(u[:, :half], u[:, half:], inv_twist[row, 2 * e], inv_twist[row, 2 * e + 1])
                )
            lows.append(jnp.concatenate([got[0][0] + got[1][0], got[0][1] + got[1][1]], 0))
            highs.append(jnp.concatenate([got[0][0] - got[1][0], got[0][1] - got[1][1]], 0))
        rows = outer // strips
        for side, value in enumerate((lows, highs)):
            high, low = split(jnp.concatenate(value, 1))
            left = last_ref[side]
            res = dot(left, high)
            res = res[: 2 * rows] + res[2 * rows :] + dot(left[: 2 * rows], low)
            for i in range(PAIR):
                place = lax.rem(step, 8 // PAIR) * PAIR + i + 8 * side
                for part in range(2):
                    out_ref[part, step // (8 // PAIR), pl.ds(place, rows, stride=16), :] = res[
                        part * rows : (part + 1) * rows, i * half : (i + 1) * half
                    ]
        return carry

    def both(step, carry):
        forward(step, 0)
        inverse(step, 0)
        return carry

    early = pairs // 2
    lax.fori_loop(0, early, forward, 0)
    for dz in range(1, blks):
        filter_copy(dz).wait_recv()
        relay_copy(dz).start()
    for dz in range(1, blks):
        relay_copy(dz).wait_recv()
    last_load.wait()
    lax.fori_loop(0, early, inverse, 0)
    lax.fori_loop(early, pairs, both, 0)

    def end_step(step, carry):
        for dt, ds in peers:
            echo_copy(step, dt, ds).wait_send()
        return carry

    lax.fori_loop(0, pairs, end_step, 0)
    for dz in range(1, blks):
        filter_copy(dz).wait_send()
        relay_copy(dz).wait_send()


def per_device(turns, blks, strips, echoes, filters, slab_index, shifts):
    sources = turns * strips
    length = filters.shape[2]
    half = LANES
    outer = length // (2 * half)
    local = outer // sources
    row_count = slab_index.shape[0]
    slab_local = filters.shape[1]
    pairs = row_count // PAIR
    shaped = echoes.reshape(2, -1, 8, 2 * local, half).transpose(0, 1, 3, 2, 4)
    response = filters.reshape(2, slab_local, 2 * outer, half).transpose(0, 2, 1, 3)
    response = response.reshape(2, -1, half)
    tables = [jnp.asarray(t) for t in make_tables(length, sources, strips)]
    hbm, smem = pl.BlockSpec(memory_space=pltpu.HBM), pl.BlockSpec(memory_space=pltpu.SMEM)
    rows = outer // strips
    image = pl.pallas_call(
        functools.partial(body, turns, blks, strips, length),
        out_shape=pltpu.VMEM((2, row_count // 8, rows * 16, half), f32),
        in_specs=[smem, smem] + [hbm] * 6,
        out_specs=pl.BlockSpec(memory_space=pltpu.VMEM),
        scratch_shapes=[
            pltpu.VMEM((pairs, sources, 2, PAIR, local, 2 * half), bf16),
            pltpu.VMEM((slab_local * blks, 2, 2, outer, half), bf16),
            pltpu.VMEM((row_count, 4, outer, half), f32),
            pltpu.VMEM((row_count, 2, 8, 2 * half), f32),
            pltpu.VMEM((pairs, 2 * PAIR * outer, 2 * half), f32),
            pltpu.VMEM(tables[0].shape, bf16),
            pltpu.VMEM(tables[1].shape, bf16),
            pltpu.VMEM(tables[2].shape, f32),
            pltpu.VMEM(tables[3].shape[1:], bf16),
            pltpu.VMEM(shaped.shape, bf16),
            pltpu.VMEM(response.shape, bf16),
            pltpu.VMEM((2, 16 * local, half), f32),
            pltpu.VMEM((turns, pairs, 2, PAIR, local, 2 * half), bf16),
            pltpu.SemaphoreType.DMA((pairs, sources)),
            pltpu.SemaphoreType.DMA((pairs, sources)),
            pltpu.SemaphoreType.DMA((blks,)),
            pltpu.SemaphoreType.DMA((blks,)),
            pltpu.SemaphoreType.DMA((blks,)),
            pltpu.SemaphoreType.DMA((blks,)),
            pltpu.SemaphoreType.DMA((6,)),
        ],
        compiler_params=pltpu.CompilerParams(
            collective_id=0, has_side_effects=True, vmem_limit_bytes=56 * 1024 * 1024
        ),
    )(shifts, slab_index, shaped, response, *tables)
    image = image.reshape(2, row_count // 8, rows * 2, 8, half).transpose(0, 1, 3, 2, 4)
    return image.reshape(2, row_count, rows * 2 * half)


def solution(mesh):
    in_specs = (
        P(None, "blk", ("turn", "strip")),
        P(None, "blk", None),
        P(("blk", "turn")),
        P(("blk", "turn")),
    )
    out_specs = P(None, ("blk", "turn"), "strip")
    local = functools.partial(
        per_device, mesh.shape["turn"], mesh.shape["blk"], mesh.shape["strip"]
    )
    return jax.shard_map(local, mesh=mesh, in_specs=in_specs, out_specs=out_specs, check_vma=False)
```

```python
import functools
import math

import jax
import jax.numpy as jnp
import numpy as np
from jax import lax
from jax.experimental import pallas as pl
from jax.experimental.pallas import tpu as pltpu
from jax.sharding import PartitionSpec as P

LANES = 128
PAIR = 2
MESH = pl.DeviceIdType.MESH
f32, bf16 = jnp.float32, jnp.bfloat16


def split_np(table):
    high = table.astype(jnp.bfloat16)
    low = (table - high.astype(np.float64)).astype(jnp.bfloat16)
    return high, low


def make_tables(length, sources, strips):
    half = LANES
    outer = length // (2 * half)
    local = outer // sources
    a_ids, c_ids = np.arange(outer), np.arange(outer)
    b_ids = np.arange(half)
    tau = np.exp(-2j * np.pi * half * c_ids / length)
    first = np.exp(-2j * np.pi * ((c_ids[:, None] * a_ids[None, :]) % outer) / outer)
    stage_one = []
    for mat in (first, tau[:, None] * first):
        grouped = mat.reshape(outer, sources, 1, local)
        top = np.concatenate([grouped.real, -grouped.imag], 2).reshape(outer, 2 * outer)
        bottom = np.concatenate([grouped.imag, grouped.real], 2).reshape(outer, 2 * outer)
        stage_one.append(np.concatenate(split_np(np.concatenate([top, bottom], 0)), 0))
    stage_one = np.stack(stage_one)
    base = np.exp(-2j * np.pi * ((b_ids[:, None] * b_ids[None, :]) % half) / half)

    def right(mat):
        whole = np.concatenate(
            [np.concatenate([mat.real, mat.imag], 1), np.concatenate([-mat.imag, mat.real], 1)], 0
        )
        high, low = split_np(whole)
        return np.concatenate([high, low, high], 0)

    stage_two = np.stack([right(base), right(base.conj())])
    twist = np.exp(-2j * np.pi * ((c_ids[:, None] * b_ids[None, :]) % length) / length)
    omega = np.exp(-2j * np.pi * b_ids / (2 * half))
    turned = twist * omega[None, :]
    twists = np.stack([twist.real, twist.imag, turned.real, turned.imag]).astype(np.float32)
    rows = outer // strips
    last = []
    for strip in range(strips):
        picked = np.arange(strip * rows, (strip + 1) * rows)
        back = np.exp(2j * np.pi * ((picked[:, None] * c_ids[None, :]) % outer) / outer) / length
        per_half = []
        for mat in (back, back * tau.conj()[None, :]):
            whole = np.concatenate(
                [np.concatenate([mat.real, -mat.imag], 1), np.concatenate([mat.imag, mat.real], 1)], 0
            )
            per_half.append(np.concatenate(split_np(whole), 0))
        last.append(np.stack(per_half))
    return stage_one, stage_two, twists, np.stack(last)


def cosine_sine(phase, length):
    quarter = length // 4
    wrapped = phase & (length - 1)
    quadrant = (wrapped + quarter // 2) // quarter if quarter & (quarter - 1) else (
        wrapped + quarter // 2
    ) >> (quarter.bit_length() - 1)
    angle = (wrapped - quadrant * quarter).astype(f32) * (2.0 * math.pi / length)
    square = angle * angle
    sine = angle * (
        1.0 + square * (-1.0 / 6 + square * (1.0 / 120 + square * (-1.0 / 5040 + square * (1.0 / 362880))))
    )
    cosine = 1.0 + square * (
        -0.5
        + square * (1.0 / 24 + square * (-1.0 / 720 + square * (1.0 / 40320 - square * (1.0 / 3628800))))
    )
    odd = (quadrant & 1) == 1
    out_cos = jnp.where(odd, sine, cosine)
    out_sin = jnp.where(odd, cosine, sine)
    quad = quadrant & 3
    out_cos = jnp.where((quad == 1) | (quad == 2), -out_cos, out_cos)
    out_sin = jnp.where(quad >= 2, -out_sin, out_sin)
    return out_cos, out_sin


def cmul(ar, ai, br, bi):
    return ar * br - ai * bi, ar * bi + ai * br


def split(values):
    high = values.astype(bf16)
    return high, (values - high.astype(f32)).astype(bf16)


def dot(left, right):
    return jnp.dot(left, right, preferred_element_type=f32)


def body(
    turns, blks, strips, length,
    shifts_ref, slabs_ref, ech_ref, filt_ref, one_hbm, two_hbm, twist_hbm, last_hbm,
    out_ref,
    recv, filt_all, inv_twist, ramp, spec, one_ref, two_ref, twist_ref, last_ref, ech_raw, filt_raw, staged, outbox,
    send_sem, recv_sem, fsend, frecv, gsend, grecv, load_sem,
):
    turn, blk, strip = lax.axis_index("turn"), lax.axis_index("blk"), lax.axis_index("strip")
    pairs = recv.shape[0]
    row_count = pairs * PAIR
    slab_local = filt_ref.shape[1] * LANES // length
    core = lax.rem(turn, 2)
    partner = turn + 1 - 2 * core
    peers = [(dt, ds) for dt in range(turns) for ds in range(strips) if (dt, ds) != (0, 0)]

    def peer(dt, ds):
        return (lax.rem(turn + dt, turns), blk, lax.rem(strip + ds, strips))

    me = turn * strips + strip
    twist_load = pltpu.make_async_copy(twist_hbm, twist_ref, load_sem.at[0])
    one_load = pltpu.make_async_copy(one_hbm, one_ref, load_sem.at[1])
    two_load = pltpu.make_async_copy(two_hbm, two_ref, load_sem.at[2])
    last_load = pltpu.make_async_copy(last_hbm.at[strip], last_ref, load_sem.at[3])
    echo_load = pltpu.make_async_copy(ech_ref, ech_raw, load_sem.at[4])
    filter_load = pltpu.make_async_copy(filt_ref, filt_raw, load_sem.at[5])
    echo_load.start()
    filter_load.start()

    barrier = pltpu.get_barrier_semaphore()
    for dt, ds in peers:
        pl.semaphore_signal(barrier, inc=1, device_id=peer(dt, ds), device_id_type=MESH)
    twist_load.start()
    one_load.start()
    two_load.start()
    last_load.start()

    def signal_blk(to):
        pl.semaphore_signal(barrier, inc=1, device_id=(turn, to, strip), device_id_type=MESH)

    def echo_copy(step, dt, ds):
        to = peer(dt, ds)
        return pltpu.make_async_remote_copy(
            src_ref=outbox.at[to[0], step],
            dst_ref=recv.at[step, me],
            send_sem=send_sem.at[0],
            recv_sem=recv_sem.at[step],
            device_id=to,
            device_id_type=MESH,
        )

    def filter_copy(dz):
        return pltpu.make_async_remote_copy(
            src_ref=filt_all.at[pl.ds(blk * slab_local, slab_local), core],
            dst_ref=filt_all.at[pl.ds(blk * slab_local, slab_local), core],
            send_sem=fsend.at[0],
            recv_sem=frecv.at[dz],
            device_id=(turn, lax.rem(blk + dz, blks), strip),
            device_id_type=MESH,
        )

    def relay_copy(dz):
        origin = lax.rem(blk + blks - dz, blks)
        place = filt_all.at[pl.ds(origin * slab_local, slab_local), core]
        return pltpu.make_async_remote_copy(
            src_ref=place,
            dst_ref=place,
            send_sem=gsend.at[0],
            recv_sem=grecv.at[0],
            device_id=(partner, blk, strip),
            device_id_type=MESH,
        )

    half = LANES
    outer = length // (2 * half)
    local = ech_raw.shape[2] // 2
    groups = row_count // 8
    per_group = 8 // PAIR

    def arrange(group):
        def fill(to, carry):
            for part in range(2):
                values = ech_raw[part, to * groups + group].astype(f32)
                staged[part] = values.reshape(2 * local * 8, half)
            for part in range(2):
                for row in range(8):
                    for side in range(2):
                        value = staged[part, pl.ds(side * 8 + row, local, stride=16), :]
                        outbox[
                            to, group * per_group + row // PAIR, part, row % PAIR, :,
                            side * half : (side + 1) * half,
                        ] = value.astype(bf16)
            return carry

        lax.fori_loop(0, turns, fill, 0)

    def send(group):
        first, end = group * per_group, (group + 1) * per_group

        def start_step(step, carry):
            for dt, ds in peers:
                echo_copy(step, dt, ds).start()
            return carry

        lax.fori_loop(first, end, start_step, 0)

        def keep(step, carry):
            recv[step, me] = outbox[turn, step]
            return carry

        lax.fori_loop(first, end, keep, 0)

    echo_load.wait()
    arrange(0)
    pl.semaphore_wait(barrier, len(peers) + jnp.where(blk > 0, 1, 0))
    send(0)

    @pl.when(blk < blks - 1)
    def _():
        signal_blk(blk + 1)

    @pl.when(blk == blks - 1)
    def _():
        signal_blk(blk - 1)

    for group in range(1, groups):
        arrange(group)
        send(group)
    filter_load.wait()
    bins = filt_raw.shape[1]
    bin_ids = lax.broadcasted_iota(jnp.int32, (bins, half), 0)
    d_ids = lax.broadcasted_iota(jnp.int32, (bins, half), 1)
    for s in range(slab_local):
        for e in range(2):
            picker = (bin_ids == (d_ids * 2 + e) * slab_local + s).astype(f32).astype(bf16)
            for part in range(2):
                got = lax.dot_general(
                    filt_raw[part], picker, (((0,), (0,)), ((), ())), preferred_element_type=f32
                )
                filt_all[blk * slab_local + s, part, e] = got.astype(bf16)
    for dz in range(1, blks):

        @pl.when(blk + dz >= blks)
        def _(dz=dz):
            filter_copy(dz).start()

    c_ids = lax.broadcasted_iota(jnp.int32, (outer, half), 0)
    lane_ids = lax.broadcasted_iota(jnp.int32, (8, 2 * half), 1)
    k_ids = jnp.where(lane_ids >= half, (lane_ids - half) * (2 * outer) + outer, lane_ids * (2 * outer))

    def prepare(row, carry):
        shift = shifts_ref[row]
        vr, vi = cosine_sine(c_ids * shift, length)
        vi = -vi
        for part in range(2):
            tr, ti = twist_ref[2 * part], -twist_ref[2 * part + 1]
            rr, ri = cmul(tr, ti, vr, vi)
            inv_twist[row, 2 * part] = rr
            inv_twist[row, 2 * part + 1] = ri
        ur, ui = cosine_sine(k_ids * shift, length)
        ramp[row, 0] = ur
        ramp[row, 1] = -ui
        return carry

    @pl.when(blk < blks - 1)
    def _():
        pl.semaphore_wait(barrier, 1)

        @pl.when(blk > 0)
        def _():
            signal_blk(blk - 1)

        for dz in range(1, blks):

            @pl.when(blk + dz < blks)
            def _(dz=dz):
                filter_copy(dz).start()

    twist_load.wait()
    lax.fori_loop(0, row_count, prepare, 0)

    one_load.wait()
    two_load.wait()

    def lefts(blocks):
        highs, lows = [], []
        for re, im in blocks:
            high, low = split(jnp.concatenate([re, im], 1))
            highs.append(high)
            lows.append(low)
        high, low = jnp.concatenate(highs, 0), jnp.concatenate(lows, 0)
        return jnp.concatenate([high, high, low], 1)

    def forward(step, carry):
        arrived = recv.at[step, pl.ds(0, len(peers))]
        pltpu.make_async_copy(arrived, arrived, recv_sem.at[step]).wait()
        rows = [recv[step, :, :, i].reshape(2 * outer, 2 * half) for i in range(PAIR)]
        parts = []
        for side in range(2):
            lanes = slice(side * half, (side + 1) * half)
            res = dot(one_ref[side], jnp.concatenate([r[:, lanes] for r in rows], 1))
            parts.append(res[: 2 * outer] + res[2 * outer :])
        total, differ = parts[0] + parts[1], parts[0] - parts[1]
        blocks = []
        for e, value in enumerate((total, differ)):
            tr, ti = twist_ref[2 * e], twist_ref[2 * e + 1]
            for i in range(PAIR):
                lanes = slice(i * half, (i + 1) * half)
                blocks.append(cmul(value[:outer, lanes], value[outer:, lanes], tr, ti))
        spec[step] = dot(lefts(blocks), two_ref[0])
        return carry

    def inverse(step, carry):
        blocks = []
        for e in range(2):
            lanes = slice(e * half, (e + 1) * half)
            for i in range(PAIR):
                row = step * PAIR + i
                picked = filt_all[slabs_ref[row], :, e].astype(f32)
                ur, ui = ramp[row, 0][:1, lanes], ramp[row, 1][:1, lanes]
                gr, gi = cmul(picked[0], picked[1], ur, ui)
                base = (e * PAIR + i) * outer
                z = spec[step, base : base + outer]
                blocks.append(cmul(z[:, :half], z[:, half:], gr, gi))
        back = dot(lefts(blocks), two_ref[1])
        lows, highs = [], []
        for i in range(PAIR):
            row = step * PAIR + i
            got = []
            for e in range(2):
                base = (e * PAIR + i) * outer
                u = back[base : base + outer]
                got.append(
                    cmul(u[:, :half], u[:, half:], inv_twist[row, 2 * e], inv_twist[row, 2 * e + 1])
                )
            lows.append(jnp.concatenate([got[0][0] + got[1][0], got[0][1] + got[1][1]], 0))
            highs.append(jnp.concatenate([got[0][0] - got[1][0], got[0][1] - got[1][1]], 0))
        rows = outer // strips
        for side, value in enumerate((lows, highs)):
            high, low = split(jnp.concatenate(value, 1))
            left = last_ref[side]
            res = dot(left, high)
            res = res[: 2 * rows] + res[2 * rows :] + dot(left[: 2 * rows], low)
            for i in range(PAIR):
                place = lax.rem(step, 8 // PAIR) * PAIR + i + 8 * side
                for part in range(2):
                    out_ref[part, step // (8 // PAIR), pl.ds(place, rows, stride=16), :] = res[
                        part * rows : (part + 1) * rows, i * half : (i + 1) * half
                    ]
        return carry

    def both(step, carry):
        forward(step, 0)
        inverse(step, 0)
        return carry

    early = pairs // 2
    lax.fori_loop(0, early, forward, 0)
    for dz in range(1, blks):
        filter_copy(dz).wait_recv()
        relay_copy(dz).start()
    others = filt_all.at[pl.ds(0, (blks - 1) * slab_local), 0]
    pltpu.make_async_copy(others, others, grecv.at[0]).wait()
    last_load.wait()
    lax.fori_loop(0, early, inverse, 0)
    lax.fori_loop(early, pairs, both, 0)

    sent = recv.at[:, pl.ds(0, len(peers))]
    pltpu.make_async_copy(sent, sent, send_sem.at[0]).wait()
    pltpu.make_async_copy(others, others, fsend.at[0]).wait()
    pltpu.make_async_copy(others, others, gsend.at[0]).wait()


def per_device(turns, blks, strips, echoes, filters, slab_index, shifts):
    sources = turns * strips
    length = filters.shape[2]
    half = LANES
    outer = length // (2 * half)
    local = outer // sources
    row_count = slab_index.shape[0]
    slab_local = filters.shape[1]
    pairs = row_count // PAIR
    shaped = echoes.reshape(2, -1, 8, 2 * local, half).transpose(0, 1, 3, 2, 4)
    response = filters.reshape(2, slab_local, 2 * outer, half).transpose(0, 2, 1, 3)
    response = response.reshape(2, -1, half)
    tables = [jnp.asarray(t) for t in make_tables(length, sources, strips)]
    hbm, smem = pl.BlockSpec(memory_space=pltpu.HBM), pl.BlockSpec(memory_space=pltpu.SMEM)
    rows = outer // strips
    image = pl.pallas_call(
        functools.partial(body, turns, blks, strips, length),
        out_shape=pltpu.VMEM((2, row_count // 8, rows * 16, half), f32),
        in_specs=[smem, smem] + [hbm] * 6,
        out_specs=pl.BlockSpec(memory_space=pltpu.VMEM),
        scratch_shapes=[
            pltpu.VMEM((pairs, sources, 2, PAIR, local, 2 * half), bf16),
            pltpu.VMEM((slab_local * blks, 2, 2, outer, half), bf16),
            pltpu.VMEM((row_count, 4, outer, half), f32),
            pltpu.VMEM((row_count, 2, 8, 2 * half), f32),
            pltpu.VMEM((pairs, 2 * PAIR * outer, 2 * half), f32),
            pltpu.VMEM(tables[0].shape, bf16),
            pltpu.VMEM(tables[1].shape, bf16),
            pltpu.VMEM(tables[2].shape, f32),
            pltpu.VMEM(tables[3].shape[1:], bf16),
            pltpu.VMEM(shaped.shape, bf16),
            pltpu.VMEM(response.shape, bf16),
            pltpu.VMEM((2, 16 * local, half), f32),
            pltpu.VMEM((turns, pairs, 2, PAIR, local, 2 * half), bf16),
            pltpu.SemaphoreType.DMA((1,)),
            pltpu.SemaphoreType.DMA((pairs,)),
            pltpu.SemaphoreType.DMA((1,)),
            pltpu.SemaphoreType.DMA((blks,)),
            pltpu.SemaphoreType.DMA((1,)),
            pltpu.SemaphoreType.DMA((1,)),
            pltpu.SemaphoreType.DMA((6,)),
        ],
        compiler_params=pltpu.CompilerParams(
            collective_id=0, has_side_effects=True, vmem_limit_bytes=56 * 1024 * 1024
        ),
    )(shifts, slab_index, shaped, response, *tables)
    image = image.reshape(2, row_count // 8, rows * 2, 8, half).transpose(0, 1, 3, 2, 4)
    return image.reshape(2, row_count, rows * 2 * half)


def solution(mesh):
    in_specs = (
        P(None, "blk", ("turn", "strip")),
        P(None, "blk", None),
        P(("blk", "turn")),
        P(("blk", "turn")),
    )
    out_specs = P(None, ("blk", "turn"), "strip")
    local = functools.partial(
        per_device, mesh.shape["turn"], mesh.shape["blk"], mesh.shape["strip"]
    )
    return jax.shard_map(local, mesh=mesh, in_specs=in_specs, out_specs=out_specs, check_vma=False)
```

```python
import functools
import math

import jax
import jax.numpy as jnp
import numpy as np
from jax import lax
from jax.experimental import pallas as pl
from jax.experimental.pallas import tpu as pltpu
from jax.sharding import PartitionSpec as P

LANES = 128
PAIR = 2
CHUNK = 64
MESH = pl.DeviceIdType.MESH
f32, bf16 = jnp.float32, jnp.bfloat16


def split_np(table):
    high = table.astype(jnp.bfloat16)
    low = (table - high.astype(np.float64)).astype(jnp.bfloat16)
    return high, low


def make_tables(length, sources, strips):
    half = LANES
    outer = length // (2 * half)
    local = outer // sources
    a_ids, c_ids = np.arange(outer), np.arange(outer)
    b_ids = np.arange(half)
    tau = np.exp(-2j * np.pi * half * c_ids / length)
    first = np.exp(-2j * np.pi * ((c_ids[:, None] * a_ids[None, :]) % outer) / outer)
    stage_one = []
    for mat in (first, tau[:, None] * first):
        grouped = mat.reshape(outer, sources, 1, local)
        top = np.concatenate([grouped.real, -grouped.imag], 2).reshape(-1, CHUNK, 2 * outer)
        bottom = np.concatenate([grouped.imag, grouped.real], 2).reshape(-1, CHUNK, 2 * outer)
        whole = np.concatenate([top, bottom], 1).reshape(2 * outer, 2 * outer)
        stage_one.append(np.concatenate(split_np(whole), 1))
    stage_one = np.stack(stage_one)
    base = np.exp(-2j * np.pi * ((b_ids[:, None] * b_ids[None, :]) % half) / half)

    def right(mat):
        whole = np.concatenate(
            [np.concatenate([mat.real, mat.imag], 1), np.concatenate([-mat.imag, mat.real], 1)], 0
        )
        high, low = split_np(whole)
        return np.concatenate([high, low, high], 0)

    stage_two = np.stack([right(base), right(base.conj())])
    twist = np.exp(-2j * np.pi * ((c_ids[:, None] * b_ids[None, :]) % length) / length)
    omega = np.exp(-2j * np.pi * b_ids / (2 * half))
    turned = twist * omega[None, :]
    twists = np.stack([twist.real, twist.imag, turned.real, turned.imag]).astype(np.float32)
    rows = outer // strips
    last = []
    for strip in range(strips):
        picked = np.arange(strip * rows, (strip + 1) * rows)
        back = np.exp(2j * np.pi * ((picked[:, None] * c_ids[None, :]) % outer) / outer) / length
        per_half = []
        for mat in (back, back * tau.conj()[None, :]):
            whole = np.concatenate(
                [np.concatenate([mat.real, -mat.imag], 1), np.concatenate([mat.imag, mat.real], 1)], 0
            )
            high, low = split_np(whole)
            per_half.append(np.concatenate([high, low, high], 1))
        last.append(np.stack(per_half))
    return stage_one, stage_two, twists, np.stack(last)


def cosine_sine(phase, length):
    quarter = length // 4
    wrapped = phase & (length - 1)
    quadrant = (wrapped + quarter // 2) // quarter if quarter & (quarter - 1) else (
        wrapped + quarter // 2
    ) >> (quarter.bit_length() - 1)
    angle = (wrapped - quadrant * quarter).astype(f32) * (2.0 * math.pi / length)
    square = angle * angle
    sine = angle * (
        1.0 + square * (-1.0 / 6 + square * (1.0 / 120 + square * (-1.0 / 5040 + square * (1.0 / 362880))))
    )
    cosine = 1.0 + square * (
        -0.5
        + square * (1.0 / 24 + square * (-1.0 / 720 + square * (1.0 / 40320 - square * (1.0 / 3628800))))
    )
    odd = (quadrant & 1) == 1
    out_cos = jnp.where(odd, sine, cosine)
    out_sin = jnp.where(odd, cosine, sine)
    quad = quadrant & 3
    out_cos = jnp.where((quad == 1) | (quad == 2), -out_cos, out_cos)
    out_sin = jnp.where(quad >= 2, -out_sin, out_sin)
    return out_cos, out_sin


def cmul(ar, ai, br, bi):
    return ar * br - ai * bi, ar * bi + ai * br


def split(values):
    high = values.astype(bf16)
    return high, (values - high.astype(f32)).astype(bf16)


def dot(left, right):
    return jnp.dot(left, right, preferred_element_type=f32)


def body(
    turns, blks, strips, length,
    shifts_ref, slabs_ref, ech_ref, filt_ref, one_hbm, two_hbm, twist_hbm, last_hbm,
    out_ref,
    recv, filt_all, inv_twist, ramp, spec, middle, one_ref, two_ref, twist_ref, last_ref, ech_raw, filt_raw, staged, outbox,
    send_sem, recv_sem, fsend, frecv, gsend, grecv, load_sem,
):
    turn, blk, strip = lax.axis_index("turn"), lax.axis_index("blk"), lax.axis_index("strip")
    pairs = recv.shape[0]
    row_count = pairs * PAIR
    slab_local = filt_ref.shape[1] * LANES // length
    core = lax.rem(turn, 2)
    partner = turn + 1 - 2 * core
    peers = [
        (dt, ds) for dt in range(turns) for ds in range(strips) if (dt, ds) != (0, 0)
    ]
    peers.sort(key=lambda p: (p[1] == 0, p[0] < 2, p))

    def peer(dt, ds):
        to = lax.rem(turn - core + (dt // 2) * 2, turns) + lax.rem(core + dt, 2)
        return (to, blk, lax.rem(strip + ds, strips))

    me = turn * strips + strip
    twist_load = pltpu.make_async_copy(twist_hbm, twist_ref, load_sem.at[0])
    one_load = pltpu.make_async_copy(one_hbm, one_ref, load_sem.at[1])
    two_load = pltpu.make_async_copy(two_hbm, two_ref, load_sem.at[2])
    last_load = pltpu.make_async_copy(last_hbm.at[strip], last_ref, load_sem.at[3])
    echo_load = pltpu.make_async_copy(ech_ref, ech_raw, load_sem.at[4])
    filter_load = pltpu.make_async_copy(filt_ref, filt_raw, load_sem.at[5])
    echo_load.start()
    filter_load.start()

    barrier = pltpu.get_barrier_semaphore()
    for dt, ds in peers:
        pl.semaphore_signal(barrier, inc=1, device_id=peer(dt, ds), device_id_type=MESH)
    twist_load.start()
    one_load.start()
    two_load.start()
    last_load.start()

    def signal_blk(to):
        pl.semaphore_signal(barrier, inc=1, device_id=(turn, to, strip), device_id_type=MESH)

    def echo_copy(step, dt, ds):
        to = peer(dt, ds)
        return pltpu.make_async_remote_copy(
            src_ref=outbox.at[to[0], step],
            dst_ref=recv.at[step, me],
            send_sem=send_sem.at[0],
            recv_sem=recv_sem.at[step],
            device_id=to,
            device_id_type=MESH,
        )

    def filter_copy(dz):
        return pltpu.make_async_remote_copy(
            src_ref=filt_all.at[pl.ds(blk * slab_local, slab_local), core],
            dst_ref=filt_all.at[pl.ds(blk * slab_local, slab_local), core],
            send_sem=fsend.at[0],
            recv_sem=frecv.at[dz],
            device_id=(turn, lax.rem(blk + dz, blks), strip),
            device_id_type=MESH,
        )

    def relay_copy(dz):
        origin = lax.rem(blk + blks - dz, blks)
        place = filt_all.at[pl.ds(origin * slab_local, slab_local), core]
        return pltpu.make_async_remote_copy(
            src_ref=place,
            dst_ref=place,
            send_sem=gsend.at[0],
            recv_sem=grecv.at[0],
            device_id=(partner, blk, strip),
            device_id_type=MESH,
        )

    half = LANES
    outer = length // (2 * half)
    local = ech_raw.shape[2] // 2
    groups = row_count // 8
    per_group = 8 // PAIR

    def arrange(group):
        def fill(to, carry):
            for part in range(2):
                values = ech_raw[part, to * groups + group].astype(f32)
                staged[part] = values.reshape(2 * local * 8, half)
            for part in range(2):
                for row in range(8):
                    for side in range(2):
                        value = staged[part, pl.ds(side * 8 + row, local, stride=16), :]
                        outbox[
                            to, group * per_group + row // PAIR, part, row % PAIR, :,
                            side * half : (side + 1) * half,
                        ] = value.astype(bf16)
            return carry

        lax.fori_loop(0, turns, fill, 0)

    def send(group):
        first, end = group * per_group, (group + 1) * per_group

        def start_step(step, carry):
            for dt, ds in peers:
                echo_copy(step, dt, ds).start()
            return carry

        lax.fori_loop(first, end, start_step, 0)

        def keep(step, carry):
            recv[step, me] = outbox[turn, step]
            return carry

        lax.fori_loop(first, end, keep, 0)

    echo_load.wait()
    arrange(0)
    pl.semaphore_wait(barrier, len(peers) + jnp.where(blk > 0, 1, 0))
    send(0)

    @pl.when(blk < blks - 1)
    def _():
        signal_blk(blk + 1)

    @pl.when(blk == blks - 1)
    def _():
        signal_blk(blk - 1)

    filter_load.wait()
    bins = filt_raw.shape[1]
    bin_ids = lax.broadcasted_iota(jnp.int32, (bins, half), 0)
    d_ids = lax.broadcasted_iota(jnp.int32, (bins, half), 1)
    for s in range(slab_local):
        for e in range(2):
            picker = (bin_ids == (d_ids * 2 + e) * slab_local + s).astype(f32).astype(bf16)
            for part in range(2):
                got = lax.dot_general(
                    filt_raw[part], picker, (((0,), (0,)), ((), ())), preferred_element_type=f32
                )
                filt_all[blk * slab_local + s, part, e] = got.astype(bf16)
    for dz in range(1, blks):

        @pl.when(blk + dz >= blks)
        def _(dz=dz):
            filter_copy(dz).start()

    for group in range(1, groups):
        arrange(group)
        send(group)
    c_ids = lax.broadcasted_iota(jnp.int32, (outer, half), 0)
    lane_ids = lax.broadcasted_iota(jnp.int32, (8, 2 * half), 1)
    k_ids = jnp.where(lane_ids >= half, (lane_ids - half) * (2 * outer) + outer, lane_ids * (2 * outer))

    def prepare(row, carry):
        shift = shifts_ref[row]
        vr, vi = cosine_sine(c_ids * shift, length)
        vi = -vi
        for part in range(2):
            tr, ti = twist_ref[2 * part], -twist_ref[2 * part + 1]
            rr, ri = cmul(tr, ti, vr, vi)
            inv_twist[row, 2 * part] = rr
            inv_twist[row, 2 * part + 1] = ri
        ur, ui = cosine_sine(k_ids * shift, length)
        ramp[row, 0] = ur
        ramp[row, 1] = -ui
        return carry

    @pl.when(blk < blks - 1)
    def _():
        pl.semaphore_wait(barrier, 1)

        @pl.when(blk > 0)
        def _():
            signal_blk(blk - 1)

        for dz in range(1, blks):

            @pl.when(blk + dz < blks)
            def _(dz=dz):
                filter_copy(dz).start()

    twist_load.wait()
    lax.fori_loop(0, row_count, prepare, 0)

    one_load.wait()
    two_load.wait()

    def lefts(blocks):
        highs, lows = [], []
        for re, im in blocks:
            high, low = split(jnp.concatenate([re, im], 1))
            highs.append(high)
            lows.append(low)
        high, low = jnp.concatenate(highs, 0), jnp.concatenate(lows, 0)
        return jnp.concatenate([high, high, low], 1)

    chunks = outer // CHUNK

    def forward(step, carry):
        arrived = recv.at[step, pl.ds(0, len(peers))]
        pltpu.make_async_copy(arrived, arrived, recv_sem.at[step]).wait()
        rows = [recv[step, :, :, i].reshape(2 * outer, 2 * half) for i in range(PAIR)]
        rights = []
        for side in range(2):
            lanes = slice(side * half, (side + 1) * half)
            right = jnp.concatenate([r[:, lanes] for r in rows], 1)
            rights.append(jnp.concatenate([right, right], 0))
        for chunk in range(chunks):
            ids = slice(chunk * CHUNK, (chunk + 1) * CHUNK)
            even, odd = [
                dot(one_ref[side, 2 * chunk * CHUNK : 2 * (chunk + 1) * CHUNK], rights[side])
                for side in range(2)
            ]
            blocks = []
            for e, value in enumerate((even + odd, even - odd)):
                tr, ti = twist_ref[2 * e, ids], twist_ref[2 * e + 1, ids]
                for i in range(PAIR):
                    lanes = slice(i * half, (i + 1) * half)
                    blocks.append(cmul(value[:CHUNK, lanes], value[CHUNK:, lanes], tr, ti))
            spec[step, chunk] = dot(lefts(blocks), two_ref[0])
        return carry

    def inverse(step, carry):
        for chunk in range(chunks):
            ids = slice(chunk * CHUNK, (chunk + 1) * CHUNK)
            blocks = []
            for e in range(2):
                lanes = slice(e * half, (e + 1) * half)
                for i in range(PAIR):
                    row = step * PAIR + i
                    picked = filt_all[slabs_ref[row], :, e, ids].astype(f32)
                    ur, ui = ramp[row, 0][:1, lanes], ramp[row, 1][:1, lanes]
                    gr, gi = cmul(picked[0], picked[1], ur, ui)
                    base = (e * PAIR + i) * CHUNK
                    z = spec[step, chunk, base : base + CHUNK]
                    blocks.append(cmul(z[:, :half], z[:, half:], gr, gi))
            back = dot(lefts(blocks), two_ref[1])
            for i in range(PAIR):
                row = step * PAIR + i
                got = []
                for e in range(2):
                    base = (e * PAIR + i) * CHUNK
                    u = back[base : base + CHUNK]
                    got.append(
                        cmul(
                            u[:, :half], u[:, half:],
                            inv_twist[row, 2 * e, ids], inv_twist[row, 2 * e + 1, ids],
                        )
                    )
                lanes = slice(i * half, (i + 1) * half)
                for part in range(2):
                    to = slice(part * outer + chunk * CHUNK, part * outer + (chunk + 1) * CHUNK)
                    for side, value in enumerate((got[0][part] + got[1][part], got[0][part] - got[1][part])):
                        high, low = split(value)
                        middle[side, 0, to, lanes] = high
                        middle[side, 1, to, lanes] = low
        return lax.fori_loop(step, step + 1, inverse_two, carry)

    def inverse_two(step, carry):
        rows = outer // strips
        for side in range(2):
            high, low = middle[side, 0], middle[side, 1]
            res = dot(last_ref[side], jnp.concatenate([high, high, low], 0))
            for i in range(PAIR):
                place = lax.rem(step, 8 // PAIR) * PAIR + i + 8 * side
                for part in range(2):
                    out_ref[part, step // (8 // PAIR), pl.ds(place, rows, stride=16), :] = res[
                        part * rows : (part + 1) * rows, i * half : (i + 1) * half
                    ]
        return carry

    def both(step, carry):
        forward(step, 0)
        inverse(step, 0)
        return carry

    early = pairs // 2
    def pass_on(j):
        origin = jnp.where(blk + j < blks, blk + j, blks - 1 - j)
        dz = lax.rem(blk - origin + blks, blks)
        filter_copy(dz).wait_recv()
        relay_copy(dz).start()

    lax.fori_loop(0, early - 1, forward, 0)
    for j in range(1, blks - 1):
        pass_on(j)
    lax.fori_loop(early - 1, early, forward, 0)
    pass_on(blks - 1)
    others = filt_all.at[pl.ds(0, (blks - 1) * slab_local), 0]
    pltpu.make_async_copy(others, others, grecv.at[0]).wait()
    last_load.wait()
    lax.fori_loop(0, early, inverse, 0)
    lax.fori_loop(early, pairs, both, 0)

    sent = recv.at[:, pl.ds(0, len(peers))]
    pltpu.make_async_copy(sent, sent, send_sem.at[0]).wait()
    pltpu.make_async_copy(others, others, fsend.at[0]).wait()
    pltpu.make_async_copy(others, others, gsend.at[0]).wait()


def per_device(turns, blks, strips, echoes, filters, slab_index, shifts):
    sources = turns * strips
    length = filters.shape[2]
    half = LANES
    outer = length // (2 * half)
    local = outer // sources
    row_count = slab_index.shape[0]
    slab_local = filters.shape[1]
    pairs = row_count // PAIR
    shaped = echoes.reshape(2, -1, 8, 2 * local, half).transpose(0, 1, 3, 2, 4)
    response = filters.reshape(2, slab_local, 2 * outer, half).transpose(0, 2, 1, 3)
    response = response.reshape(2, -1, half)
    tables = [jnp.asarray(t) for t in make_tables(length, sources, strips)]
    hbm, smem = pl.BlockSpec(memory_space=pltpu.HBM), pl.BlockSpec(memory_space=pltpu.SMEM)
    rows = outer // strips
    image = pl.pallas_call(
        functools.partial(body, turns, blks, strips, length),
        out_shape=pltpu.VMEM((2, row_count // 8, rows * 16, half), f32),
        in_specs=[smem, smem] + [hbm] * 6,
        out_specs=pl.BlockSpec(memory_space=pltpu.VMEM),
        scratch_shapes=[
            pltpu.VMEM((pairs, sources, 2, PAIR, local, 2 * half), bf16),
            pltpu.VMEM((slab_local * blks, 2, 2, outer, half), bf16),
            pltpu.VMEM((row_count, 4, outer, half), f32),
            pltpu.VMEM((row_count, 2, 8, 2 * half), f32),
            pltpu.VMEM((pairs, outer // CHUNK, 2 * PAIR * CHUNK, 2 * half), f32),
            pltpu.VMEM((2, 2, 2 * outer, 2 * half), bf16),
            pltpu.VMEM(tables[0].shape, bf16),
            pltpu.VMEM(tables[1].shape, bf16),
            pltpu.VMEM(tables[2].shape, f32),
            pltpu.VMEM(tables[3].shape[1:], bf16),
            pltpu.VMEM(shaped.shape, bf16),
            pltpu.VMEM(response.shape, bf16),
            pltpu.VMEM((2, 16 * local, half), f32),
            pltpu.VMEM((turns, pairs, 2, PAIR, local, 2 * half), bf16),
            pltpu.SemaphoreType.DMA((1,)),
            pltpu.SemaphoreType.DMA((pairs,)),
            pltpu.SemaphoreType.DMA((1,)),
            pltpu.SemaphoreType.DMA((blks,)),
            pltpu.SemaphoreType.DMA((1,)),
            pltpu.SemaphoreType.DMA((1,)),
            pltpu.SemaphoreType.DMA((6,)),
        ],
        compiler_params=pltpu.CompilerParams(
            collective_id=0, has_side_effects=True, vmem_limit_bytes=56 * 1024 * 1024
        ),
    )(shifts, slab_index, shaped, response, *tables)
    image = image.reshape(2, row_count // 8, rows * 2, 8, half).transpose(0, 1, 3, 2, 4)
    return image.reshape(2, row_count, rows * 2 * half)


def solution(mesh):
    in_specs = (
        P(None, "blk", ("turn", "strip")),
        P(None, "blk", None),
        P(("blk", "turn")),
        P(("blk", "turn")),
    )
    out_specs = P(None, ("blk", "turn"), "strip")
    local = functools.partial(
        per_device, mesh.shape["turn"], mesh.shape["blk"], mesh.shape["strip"]
    )
    return jax.shard_map(local, mesh=mesh, in_specs=in_specs, out_specs=out_specs, check_vma=False)
```

```python
import functools
import math

import jax
import jax.numpy as jnp
import numpy as np
from jax import lax
from jax.experimental import pallas as pl
from jax.experimental.pallas import tpu as pltpu
from jax.sharding import PartitionSpec as P

LANES = 128
PAIR = 2
CHUNK = 64
BACK = 32
MESH = pl.DeviceIdType.MESH
f32, bf16 = jnp.float32, jnp.bfloat16


def split_np(table):
    high = table.astype(jnp.bfloat16)
    low = (table - high.astype(np.float64)).astype(jnp.bfloat16)
    return high, low


def make_tables(length, sources, strips):
    half = LANES
    outer = length // (2 * half)
    local = outer // sources
    a_ids, c_ids = np.arange(outer), np.arange(outer)
    b_ids = np.arange(half)
    tau = np.exp(-2j * np.pi * half * c_ids / length)
    first = np.exp(-2j * np.pi * ((c_ids[:, None] * a_ids[None, :]) % outer) / outer)
    stage_one = []
    for mat in (first, tau[:, None] * first):
        grouped = mat.reshape(outer, sources, 1, local)
        top = np.concatenate([grouped.real, -grouped.imag], 2).reshape(-1, CHUNK, 2 * outer)
        bottom = np.concatenate([grouped.imag, grouped.real], 2).reshape(-1, CHUNK, 2 * outer)
        whole = np.concatenate([top, bottom], 1).reshape(2 * outer, 2 * outer)
        stage_one.append(np.concatenate(split_np(whole), 1))
    stage_one = np.stack(stage_one)
    base = np.exp(-2j * np.pi * ((b_ids[:, None] * b_ids[None, :]) % half) / half)

    def right(mat):
        whole = np.concatenate(
            [np.concatenate([mat.real, mat.imag], 1), np.concatenate([-mat.imag, mat.real], 1)], 0
        )
        high, low = split_np(whole)
        return np.concatenate([high, low, high], 0)

    stage_two = np.stack([right(base), right(base.conj())])
    twist = np.exp(-2j * np.pi * ((c_ids[:, None] * b_ids[None, :]) % length) / length)
    omega = np.exp(-2j * np.pi * b_ids / (2 * half))
    turned = twist * omega[None, :]
    twists = np.stack([twist.real, twist.imag, turned.real, turned.imag]).astype(np.float32)
    rows = outer // strips
    last = []
    for strip in range(strips):
        picked = np.arange(strip * rows, (strip + 1) * rows)
        back = np.exp(2j * np.pi * ((picked[:, None] * c_ids[None, :]) % outer) / outer) / length
        per_half = []
        for mat in (back, back * tau.conj()[None, :]):
            whole = np.concatenate(
                [np.concatenate([mat.real, -mat.imag], 1), np.concatenate([mat.imag, mat.real], 1)], 0
            )
            high, low = split_np(whole)
            per_half.append(np.concatenate([high, low, high], 1))
        last.append(np.stack(per_half))
    return stage_one, stage_two, twists, np.stack(last)


def cosine_sine(phase, length):
    quarter = length // 4
    wrapped = phase & (length - 1)
    quadrant = (wrapped + quarter // 2) // quarter if quarter & (quarter - 1) else (
        wrapped + quarter // 2
    ) >> (quarter.bit_length() - 1)
    angle = (wrapped - quadrant * quarter).astype(f32) * (2.0 * math.pi / length)
    square = angle * angle
    sine = angle * (
        1.0 + square * (-1.0 / 6 + square * (1.0 / 120 + square * (-1.0 / 5040 + square * (1.0 / 362880))))
    )
    cosine = 1.0 + square * (
        -0.5
        + square * (1.0 / 24 + square * (-1.0 / 720 + square * (1.0 / 40320 - square * (1.0 / 3628800))))
    )
    odd = (quadrant & 1) == 1
    out_cos = jnp.where(odd, sine, cosine)
    out_sin = jnp.where(odd, cosine, sine)
    quad = quadrant & 3
    out_cos = jnp.where((quad == 1) | (quad == 2), -out_cos, out_cos)
    out_sin = jnp.where(quad >= 2, -out_sin, out_sin)
    return out_cos, out_sin


def cmul(ar, ai, br, bi):
    return ar * br - ai * bi, ar * bi + ai * br


def split(values):
    high = values.astype(bf16)
    return high, (values - high.astype(f32)).astype(bf16)


def dot(left, right):
    return jnp.dot(left, right, preferred_element_type=f32)


def body(
    turns, blks, strips, length,
    shifts_ref, slabs_ref, ech_ref, filt_ref, one_hbm, two_hbm, twist_hbm, last_hbm,
    out_ref,
    recv, filt_all, inv_twist, ramp, spec, middle, one_ref, two_ref, twist_ref, last_ref, ech_raw, filt_raw, staged, outbox,
    send_sem, recv_sem, fsend, frecv, gsend, grecv, load_sem,
):
    turn, blk, strip = lax.axis_index("turn"), lax.axis_index("blk"), lax.axis_index("strip")
    pairs = recv.shape[0]
    row_count = pairs * PAIR
    slab_local = filt_ref.shape[1] * LANES // length
    core = lax.rem(turn, 2)
    partner = turn + 1 - 2 * core
    peers = [
        (dt, ds) for dt in range(turns) for ds in range(strips) if (dt, ds) != (0, 0)
    ]
    peers.sort(key=lambda p: (p[1] == 0, p[0] < 2, p))

    def peer(dt, ds):
        to = lax.rem(turn - core + (dt // 2) * 2, turns) + lax.rem(core + dt, 2)
        return (to, blk, lax.rem(strip + ds, strips))

    me = turn * strips + strip
    twist_load = pltpu.make_async_copy(twist_hbm, twist_ref, load_sem.at[0])
    one_load = pltpu.make_async_copy(one_hbm, one_ref, load_sem.at[1])
    two_load = pltpu.make_async_copy(two_hbm, two_ref, load_sem.at[2])
    last_load = pltpu.make_async_copy(last_hbm.at[strip], last_ref, load_sem.at[3])
    filter_load = pltpu.make_async_copy(filt_ref, filt_raw, load_sem.at[5])
    groups = row_count // 8
    per_group = 8 // PAIR

    def load_group(group):
        for to in range(turns):
            block = pl.ds(to * groups + group, 1)
            pltpu.make_async_copy(
                ech_ref.at[:, block], ech_raw.at[:, block], load_sem.at[6 + group]
            ).start()

    load_group(0)
    filter_load.start()

    barrier = pltpu.get_barrier_semaphore()
    for dt, ds in peers:
        pl.semaphore_signal(barrier, inc=1, device_id=peer(dt, ds), device_id_type=MESH)
    def signal_blk(to):
        pl.semaphore_signal(barrier, inc=1, device_id=(turn, to, strip), device_id_type=MESH)

    def echo_copy(step, dt, ds):
        to = peer(dt, ds)
        return pltpu.make_async_remote_copy(
            src_ref=outbox.at[to[0], step],
            dst_ref=recv.at[step, me],
            send_sem=send_sem.at[0],
            recv_sem=recv_sem.at[step],
            device_id=to,
            device_id_type=MESH,
        )

    def filter_copy(dz):
        return pltpu.make_async_remote_copy(
            src_ref=filt_all.at[pl.ds(blk * slab_local, slab_local), core],
            dst_ref=filt_all.at[pl.ds(blk * slab_local, slab_local), core],
            send_sem=fsend.at[0],
            recv_sem=frecv.at[dz],
            device_id=(turn, lax.rem(blk + dz, blks), strip),
            device_id_type=MESH,
        )

    def relay_copy(dz):
        origin = lax.rem(blk + blks - dz, blks)
        place = filt_all.at[pl.ds(origin * slab_local, slab_local), core]
        return pltpu.make_async_remote_copy(
            src_ref=place,
            dst_ref=place,
            send_sem=gsend.at[0],
            recv_sem=grecv.at[0],
            device_id=(partner, blk, strip),
            device_id_type=MESH,
        )

    half = LANES
    outer = length // (2 * half)
    local = ech_raw.shape[2] // 2
    def stage(group):
        whole = ech_raw.at[:, pl.ds(0, turns)]
        pltpu.make_async_copy(whole, whole, load_sem.at[6 + group]).wait()

        def fill(to, carry):
            for part in range(2):
                values = ech_raw[part, to * groups + group].astype(f32)
                staged[to, part] = values.reshape(2 * local * 8, half)
            return carry

        lax.fori_loop(0, turns, fill, 0)

    def pick(step):
        first = lax.rem(step, per_group) * PAIR

        def fill(to, carry):
            for part in range(2):
                for row in range(PAIR):
                    for side in range(2):
                        value = staged[to, part, pl.ds(first + side * 8 + row, local, stride=16), :]
                        outbox[
                            to, step, part, row, :, side * half : (side + 1) * half
                        ] = value.astype(bf16)
            return carry

        lax.fori_loop(0, turns, fill, 0)

    def send(step):
        for dt, ds in peers:
            echo_copy(step, dt, ds).start()
        recv[step, me] = outbox[turn, step]

    def pick_send(step, carry):
        pick(step)
        send(step)
        return carry

    stage(0)
    for group in range(1, groups):
        load_group(group)
    pick(0)
    pl.semaphore_wait(barrier, len(peers) + jnp.where(blk > 0, 1, 0))
    send(0)

    @pl.when(blk < blks - 1)
    def _():
        signal_blk(blk + 1)

    @pl.when(blk == blks - 1)
    def _():
        signal_blk(blk - 1)

    filter_load.wait()
    bins = filt_raw.shape[1]
    bin_ids = lax.broadcasted_iota(jnp.int32, (bins, half), 0)
    d_ids = lax.broadcasted_iota(jnp.int32, (bins, half), 1)
    for s in range(slab_local):
        for e in range(2):
            picker = (bin_ids == (d_ids * 2 + e) * slab_local + s).astype(f32).astype(bf16)
            for part in range(2):
                got = lax.dot_general(
                    filt_raw[part], picker, (((0,), (0,)), ((), ())), preferred_element_type=f32
                )
                filt_all[blk * slab_local + s, part, e] = got.astype(bf16)
    for dz in range(1, blks):

        @pl.when(blk + dz >= blks)
        def _(dz=dz):
            filter_copy(dz).start()

    lax.fori_loop(1, per_group, pick_send, 0)
    twist_load.start()
    one_load.start()
    two_load.start()
    last_load.start()

    for group in range(1, groups):
        stage(group)
        lax.fori_loop(group * per_group, (group + 1) * per_group, pick_send, 0)
    c_ids = lax.broadcasted_iota(jnp.int32, (outer, half), 0)
    lane_ids = lax.broadcasted_iota(jnp.int32, (8, 2 * half), 1)
    k_ids = jnp.where(lane_ids >= half, (lane_ids - half) * (2 * outer) + outer, lane_ids * (2 * outer))

    def prepare(row, carry):
        shift = shifts_ref[row]
        vr, vi = cosine_sine(c_ids * shift, length)
        vi = -vi
        for part in range(2):
            tr, ti = twist_ref[2 * part], -twist_ref[2 * part + 1]
            rr, ri = cmul(tr, ti, vr, vi)
            inv_twist[row, 2 * part] = rr
            inv_twist[row, 2 * part + 1] = ri
        ur, ui = cosine_sine(k_ids * shift, length)
        ramp[row, 0] = ur
        ramp[row, 1] = -ui
        return carry

    @pl.when(blk < blks - 1)
    def _():
        pl.semaphore_wait(barrier, 1)

        @pl.when(blk > 0)
        def _():
            signal_blk(blk - 1)

        for dz in range(1, blks):

            @pl.when(blk + dz < blks)
            def _(dz=dz):
                filter_copy(dz).start()

    twist_load.wait()
    lax.fori_loop(0, row_count, prepare, 0)

    one_load.wait()
    two_load.wait()

    def lefts(blocks):
        highs, lows = [], []
        for re, im in blocks:
            high, low = split(jnp.concatenate([re, im], 1))
            highs.append(high)
            lows.append(low)
        high, low = jnp.concatenate(highs, 0), jnp.concatenate(lows, 0)
        return jnp.concatenate([high, high, low], 1)

    chunks = outer // CHUNK

    def forward_rows(step, picks):
        rows = [recv[step, :, :, i].reshape(2 * outer, 2 * half) for i in picks]
        rights = []
        for side in range(2):
            lanes = slice(side * half, (side + 1) * half)
            right = jnp.concatenate([r[:, lanes] for r in rows], 1)
            rights.append(jnp.concatenate([right, right], 0))
        for chunk in range(chunks):
            ids = slice(chunk * CHUNK, (chunk + 1) * CHUNK)
            even, odd = [
                dot(one_ref[side, 2 * chunk * CHUNK : 2 * (chunk + 1) * CHUNK], rights[side])
                for side in range(2)
            ]
            blocks = []
            for e, value in enumerate((even + odd, even - odd)):
                tr, ti = twist_ref[2 * e, ids], twist_ref[2 * e + 1, ids]
                for k in range(len(picks)):
                    lanes = slice(k * half, (k + 1) * half)
                    blocks.append(cmul(value[:CHUNK, lanes], value[CHUNK:, lanes], tr, ti))
            got = dot(lefts(blocks), two_ref[0])
            for e in range(2):
                for k, i in enumerate(picks):
                    base = (e * len(picks) + k) * CHUNK
                    spec[step, chunk, e, i] = got[base : base + CHUNK]

    def forward(step, carry):
        arrived = recv.at[step, pl.ds(0, len(peers))]
        pltpu.make_async_copy(arrived, arrived, recv_sem.at[step]).wait()
        forward_rows(step, range(PAIR))
        return carry

    def inverse_rows(step, picks):
        count = len(picks)
        for chunk in range(outer // BACK):
            ids = slice(chunk * BACK, (chunk + 1) * BACK)
            first = chunk * BACK % CHUNK
            blocks = []
            for e in range(2):
                lanes = slice(e * half, (e + 1) * half)
                for i in picks:
                    row = step * PAIR + i
                    picked = filt_all[slabs_ref[row], :, e, ids].astype(f32)
                    ur, ui = ramp[row, 0][:1, lanes], ramp[row, 1][:1, lanes]
                    gr, gi = cmul(picked[0], picked[1], ur, ui)
                    z = spec[step, chunk * BACK // CHUNK, e, i, first : first + BACK]
                    blocks.append(cmul(z[:, :half], z[:, half:], gr, gi))
            back = dot(lefts(blocks), two_ref[1])
            for k, i in enumerate(picks):
                row = step * PAIR + i
                got = []
                for e in range(2):
                    base = (e * count + k) * BACK
                    u = back[base : base + BACK]
                    got.append(
                        cmul(
                            u[:, :half], u[:, half:],
                            inv_twist[row, 2 * e, ids], inv_twist[row, 2 * e + 1, ids],
                        )
                    )
                lanes = slice(k * half, (k + 1) * half)
                for part in range(2):
                    to = slice(part * outer + chunk * BACK, part * outer + (chunk + 1) * BACK)
                    for side, value in enumerate((got[0][part] + got[1][part], got[0][part] - got[1][part])):
                        high, low = split(value)
                        middle[side, 0, to, lanes] = high
                        middle[side, 1, to, lanes] = low

    def image_rows(step, picks):
        rows = outer // strips
        width = len(picks) * half
        for side in range(2):
            high, low = middle[side, 0, :, :width], middle[side, 1, :, :width]
            res = dot(last_ref[side], jnp.concatenate([high, high, low], 0))
            for k, i in enumerate(picks):
                place = lax.rem(step, 8 // PAIR) * PAIR + i + 8 * side
                for part in range(2):
                    out_ref[part, step // (8 // PAIR), pl.ds(place, rows, stride=16), :] = res[
                        part * rows : (part + 1) * rows, k * half : (k + 1) * half
                    ]

    def inverse(step, carry):
        inverse_rows(step, range(PAIR))
        return lax.fori_loop(step, step + 1, image, carry)

    def image(step, carry):
        image_rows(step, range(PAIR))
        return carry

    def both(step, carry):
        forward(step, 0)
        inverse(step, 0)
        return carry

    early = pairs // 2
    def pass_on(j):
        origin = jnp.where(blk + j < blks, blk + j, blks - 1 - j)
        dz = lax.rem(blk - origin + blks, blks)
        filter_copy(dz).wait_recv()
        relay_copy(dz).start()

    lax.fori_loop(0, early - 1, forward, 0)
    for j in range(1, blks - 1):
        pass_on(j)
    lax.fori_loop(early - 1, early, forward, 0)
    pass_on(blks - 1)
    others = filt_all.at[pl.ds(0, (blks - 1) * slab_local), 0]
    pltpu.make_async_copy(others, others, grecv.at[0]).wait()
    last_load.wait()
    lax.fori_loop(0, early, inverse, 0)
    lax.fori_loop(early, pairs, both, 0)

    sent = recv.at[:, pl.ds(0, len(peers))]
    pltpu.make_async_copy(sent, sent, send_sem.at[0]).wait()
    pltpu.make_async_copy(others, others, fsend.at[0]).wait()
    pltpu.make_async_copy(others, others, gsend.at[0]).wait()


def per_device(turns, blks, strips, echoes, filters, slab_index, shifts):
    sources = turns * strips
    length = filters.shape[2]
    half = LANES
    outer = length // (2 * half)
    local = outer // sources
    row_count = slab_index.shape[0]
    slab_local = filters.shape[1]
    pairs = row_count // PAIR
    shaped = echoes.reshape(2, -1, 8, 2 * local, half).transpose(0, 1, 3, 2, 4)
    response = filters.reshape(2, slab_local, 2 * outer, half).transpose(0, 2, 1, 3)
    response = response.reshape(2, -1, half)
    tables = [jnp.asarray(t) for t in make_tables(length, sources, strips)]
    hbm, smem = pl.BlockSpec(memory_space=pltpu.HBM), pl.BlockSpec(memory_space=pltpu.SMEM)
    rows = outer // strips
    image = pl.pallas_call(
        functools.partial(body, turns, blks, strips, length),
        out_shape=pltpu.VMEM((2, row_count // 8, rows * 16, half), f32),
        in_specs=[smem, smem] + [hbm] * 6,
        out_specs=pl.BlockSpec(memory_space=pltpu.VMEM),
        scratch_shapes=[
            pltpu.VMEM((pairs, sources, 2, PAIR, local, 2 * half), bf16),
            pltpu.VMEM((slab_local * blks, 2, 2, outer, half), bf16),
            pltpu.VMEM((row_count, 4, outer, half), f32),
            pltpu.VMEM((row_count, 2, 8, 2 * half), f32),
            pltpu.VMEM((pairs, outer // CHUNK, 2, PAIR, CHUNK, 2 * half), f32),
            pltpu.VMEM((2, 2, 2 * outer, 2 * half), bf16),
            pltpu.VMEM(tables[0].shape, bf16),
            pltpu.VMEM(tables[1].shape, bf16),
            pltpu.VMEM(tables[2].shape, f32),
            pltpu.VMEM(tables[3].shape[1:], bf16),
            pltpu.VMEM(shaped.shape, bf16),
            pltpu.VMEM(response.shape, bf16),
            pltpu.VMEM((turns, 2, 16 * local, half), f32),
            pltpu.VMEM((turns, pairs, 2, PAIR, local, 2 * half), bf16),
            pltpu.SemaphoreType.DMA((1,)),
            pltpu.SemaphoreType.DMA((pairs,)),
            pltpu.SemaphoreType.DMA((1,)),
            pltpu.SemaphoreType.DMA((blks,)),
            pltpu.SemaphoreType.DMA((1,)),
            pltpu.SemaphoreType.DMA((1,)),
            pltpu.SemaphoreType.DMA((6 + row_count // 8,)),
        ],
        compiler_params=pltpu.CompilerParams(
            collective_id=0, has_side_effects=True, vmem_limit_bytes=56 * 1024 * 1024
        ),
    )(shifts, slab_index, shaped, response, *tables)
    image = image.reshape(2, row_count // 8, rows * 2, 8, half).transpose(0, 1, 3, 2, 4)
    return image.reshape(2, row_count, rows * 2 * half)


def solution(mesh):
    in_specs = (
        P(None, "blk", ("turn", "strip")),
        P(None, "blk", None),
        P(("blk", "turn")),
        P(("blk", "turn")),
    )
    out_specs = P(None, ("blk", "turn"), "strip")
    local = functools.partial(
        per_device, mesh.shape["turn"], mesh.shape["blk"], mesh.shape["strip"]
    )
    return jax.shard_map(local, mesh=mesh, in_specs=in_specs, out_specs=out_specs, check_vma=False)
```

```python
import functools
import math

import jax
import jax.numpy as jnp
import numpy as np
from jax import lax
from jax.experimental import pallas as pl
from jax.experimental.pallas import tpu as pltpu
from jax.sharding import PartitionSpec as P

LANES = 128
PAIR = 2
CHUNK = 64
BACK = 32
MESH = pl.DeviceIdType.MESH
f32, bf16 = jnp.float32, jnp.bfloat16


def split_np(table):
    high = table.astype(jnp.bfloat16)
    low = (table - high.astype(np.float64)).astype(jnp.bfloat16)
    return high, low


def make_tables(length, sources, strips):
    half = LANES
    outer = length // (2 * half)
    local = outer // sources
    a_ids, c_ids = np.arange(outer), np.arange(outer)
    b_ids = np.arange(half)
    tau = np.exp(-2j * np.pi * half * c_ids / length)
    first = np.exp(-2j * np.pi * ((c_ids[:, None] * a_ids[None, :]) % outer) / outer)
    stage_one = []
    for mat in (first, tau[:, None] * first):
        grouped = mat.reshape(outer, sources, 1, local)
        top = np.concatenate([grouped.real, -grouped.imag], 2).reshape(-1, CHUNK, 2 * outer)
        bottom = np.concatenate([grouped.imag, grouped.real], 2).reshape(-1, CHUNK, 2 * outer)
        whole = np.concatenate([top, bottom], 1).reshape(2 * outer, 2 * outer)
        stage_one.append(np.concatenate(split_np(whole), 1))
    stage_one = np.stack(stage_one)
    base = np.exp(-2j * np.pi * ((b_ids[:, None] * b_ids[None, :]) % half) / half)

    def right(mat):
        whole = np.concatenate(
            [np.concatenate([mat.real, mat.imag], 1), np.concatenate([-mat.imag, mat.real], 1)], 0
        )
        high, low = split_np(whole)
        return np.concatenate([high, low, high], 0)

    stage_two = np.stack([right(base), right(base.conj())])
    twist = np.exp(-2j * np.pi * ((c_ids[:, None] * b_ids[None, :]) % length) / length)
    omega = np.exp(-2j * np.pi * b_ids / (2 * half))
    turned = twist * omega[None, :]
    twists = np.stack([twist.real, twist.imag, turned.real, turned.imag]).astype(np.float32)
    rows = outer // strips
    last = []
    for strip in range(strips):
        picked = np.arange(strip * rows, (strip + 1) * rows)
        back = np.exp(2j * np.pi * ((picked[:, None] * c_ids[None, :]) % outer) / outer) / length
        per_half = []
        for mat in (back, back * tau.conj()[None, :]):
            whole = np.concatenate(
                [np.concatenate([mat.real, -mat.imag], 1), np.concatenate([mat.imag, mat.real], 1)], 0
            )
            high, low = split_np(whole)
            per_half.append(np.concatenate([high, low, high], 1))
        last.append(np.stack(per_half))
    return stage_one, stage_two, twists, np.stack(last)


def cosine_sine(phase, length):
    quarter = length // 4
    wrapped = phase & (length - 1)
    quadrant = (wrapped + quarter // 2) // quarter if quarter & (quarter - 1) else (
        wrapped + quarter // 2
    ) >> (quarter.bit_length() - 1)
    angle = (wrapped - quadrant * quarter).astype(f32) * (2.0 * math.pi / length)
    square = angle * angle
    sine = angle * (
        1.0 + square * (-1.0 / 6 + square * (1.0 / 120 + square * (-1.0 / 5040 + square * (1.0 / 362880))))
    )
    cosine = 1.0 + square * (
        -0.5
        + square * (1.0 / 24 + square * (-1.0 / 720 + square * (1.0 / 40320 - square * (1.0 / 3628800))))
    )
    odd = (quadrant & 1) == 1
    out_cos = jnp.where(odd, sine, cosine)
    out_sin = jnp.where(odd, cosine, sine)
    quad = quadrant & 3
    out_cos = jnp.where((quad == 1) | (quad == 2), -out_cos, out_cos)
    out_sin = jnp.where(quad >= 2, -out_sin, out_sin)
    return out_cos, out_sin


def cmul(ar, ai, br, bi):
    return ar * br - ai * bi, ar * bi + ai * br


def split(values):
    high = values.astype(bf16)
    return high, (values - high.astype(f32)).astype(bf16)


def dot(left, right):
    return jnp.dot(left, right, preferred_element_type=f32)


def body(
    turns, blks, strips, length,
    shifts_ref, slabs_ref, ech_ref, filt_ref, one_hbm, two_hbm, twist_hbm, last_hbm,
    out_ref,
    recv, filt_all, inv_twist, ramp, spec, middle, one_ref, two_ref, twist_ref, last_ref, ech_raw, filt_raw, staged, outbox,
    send_sem, recv_sem, fsend, frecv, gsend, grecv, load_sem,
):
    turn, blk, strip = lax.axis_index("turn"), lax.axis_index("blk"), lax.axis_index("strip")
    pairs = recv.shape[0]
    row_count = pairs * PAIR
    slab_local = filt_ref.shape[1] * LANES // length
    core = lax.rem(turn, 2)
    partner = turn + 1 - 2 * core
    peers = [
        (dt, ds) for dt in range(turns) for ds in range(strips) if (dt, ds) != (0, 0)
    ]
    peers.sort(key=lambda p: (p[1] == 0, p[0] % 2, p[0] < 2, p))

    def peer(dt, ds):
        to = lax.rem(turn - core + (dt // 2) * 2, turns) + lax.rem(core + dt, 2)
        return (to, blk, lax.rem(strip + ds, strips))

    me = turn * strips + strip
    twist_load = pltpu.make_async_copy(twist_hbm, twist_ref, load_sem.at[0])
    one_load = pltpu.make_async_copy(one_hbm, one_ref, load_sem.at[1])
    two_load = pltpu.make_async_copy(two_hbm, two_ref, load_sem.at[2])
    last_load = pltpu.make_async_copy(last_hbm.at[strip], last_ref, load_sem.at[3])
    filter_load = pltpu.make_async_copy(filt_ref, filt_raw, load_sem.at[5])
    groups = row_count // 8
    per_group = 8 // PAIR

    def load_group(group):
        for to in range(turns):
            block = pl.ds(to * groups + group, 1)
            pltpu.make_async_copy(
                ech_ref.at[:, block], ech_raw.at[:, block], load_sem.at[6 + group]
            ).start()

    load_group(0)
    filter_load.start()

    barrier = pltpu.get_barrier_semaphore()
    for dt, ds in peers:
        pl.semaphore_signal(barrier, inc=1, device_id=peer(dt, ds), device_id_type=MESH)
    def signal_blk(to):
        pl.semaphore_signal(barrier, inc=1, device_id=(turn, to, strip), device_id_type=MESH)

    def echo_copy(step, dt, ds):
        to = peer(dt, ds)
        return pltpu.make_async_remote_copy(
            src_ref=outbox.at[to[0], step],
            dst_ref=recv.at[step, me],
            send_sem=send_sem.at[0],
            recv_sem=recv_sem.at[step],
            device_id=to,
            device_id_type=MESH,
        )

    def filter_copy(dz):
        return pltpu.make_async_remote_copy(
            src_ref=filt_all.at[pl.ds(blk * slab_local, slab_local), core],
            dst_ref=filt_all.at[pl.ds(blk * slab_local, slab_local), core],
            send_sem=fsend.at[0],
            recv_sem=frecv.at[dz],
            device_id=(turn, lax.rem(blk + dz, blks), strip),
            device_id_type=MESH,
        )

    def relay_copy(dz):
        origin = lax.rem(blk + blks - dz, blks)
        place = filt_all.at[pl.ds(origin * slab_local, slab_local), core]
        return pltpu.make_async_remote_copy(
            src_ref=place,
            dst_ref=place,
            send_sem=gsend.at[0],
            recv_sem=grecv.at[0],
            device_id=(partner, blk, strip),
            device_id_type=MESH,
        )

    half = LANES
    outer = length // (2 * half)
    local = ech_raw.shape[2] // 2
    def stage(group):
        whole = ech_raw.at[:, pl.ds(0, turns)]
        pltpu.make_async_copy(whole, whole, load_sem.at[6 + group]).wait()

        def fill(to, carry):
            for part in range(2):
                values = ech_raw[part, to * groups + group].astype(f32)
                staged[to, part] = values.reshape(2 * local * 8, half)
            return carry

        lax.fori_loop(0, turns, fill, 0)

    def pick(step):
        first = lax.rem(step, per_group) * PAIR

        def fill(to, carry):
            for part in range(2):
                for row in range(PAIR):
                    for side in range(2):
                        value = staged[to, part, pl.ds(first + side * 8 + row, local, stride=16), :]
                        outbox[
                            to, step, part, row, :, side * half : (side + 1) * half
                        ] = value.astype(bf16)
            return carry

        lax.fori_loop(0, turns, fill, 0)

    def send(step):
        for dt, ds in peers:
            echo_copy(step, dt, ds).start()
        recv[step, me] = outbox[turn, step]

    def pick_send(step, carry):
        pick(step)
        send(step)
        return carry

    stage(0)
    for group in range(1, groups):
        load_group(group)
    pick(0)
    pl.semaphore_wait(barrier, len(peers) + jnp.where(blk > 0, 1, 0))
    send(0)

    @pl.when(blk < blks - 1)
    def _():
        signal_blk(blk + 1)

    @pl.when(blk == blks - 1)
    def _():
        signal_blk(blk - 1)

    filter_load.wait()
    bins = filt_raw.shape[1]
    bin_ids = lax.broadcasted_iota(jnp.int32, (bins, half), 0)
    d_ids = lax.broadcasted_iota(jnp.int32, (bins, half), 1)
    for s in range(slab_local):
        for e in range(2):
            picker = (bin_ids == (d_ids * 2 + e) * slab_local + s).astype(f32).astype(bf16)
            for part in range(2):
                got = lax.dot_general(
                    filt_raw[part], picker, (((0,), (0,)), ((), ())), preferred_element_type=f32
                )
                filt_all[blk * slab_local + s, part, e] = got.astype(bf16)
    for dz in range(1, blks):

        @pl.when(blk + dz >= blks)
        def _(dz=dz):
            filter_copy(dz).start()

    lax.fori_loop(1, per_group, pick_send, 0)
    twist_load.start()
    one_load.start()
    two_load.start()
    last_load.start()

    @pl.when(blk < blks - 1)
    def _():
        pl.semaphore_wait(barrier, 1)

        @pl.when(blk > 0)
        def _():
            signal_blk(blk - 1)

        for dz in range(1, blks):

            @pl.when(blk + dz < blks)
            def _(dz=dz):
                filter_copy(dz).start()

    for group in range(1, groups):
        stage(group)
        lax.fori_loop(group * per_group, (group + 1) * per_group, pick_send, 0)
    c_ids = lax.broadcasted_iota(jnp.int32, (outer, half), 0)
    lane_ids = lax.broadcasted_iota(jnp.int32, (8, 2 * half), 1)
    k_ids = jnp.where(lane_ids >= half, (lane_ids - half) * (2 * outer) + outer, lane_ids * (2 * outer))

    def prepare(row, carry):
        shift = shifts_ref[row]
        vr, vi = cosine_sine(c_ids * shift, length)
        vi = -vi
        for part in range(2):
            tr, ti = twist_ref[2 * part], -twist_ref[2 * part + 1]
            rr, ri = cmul(tr, ti, vr, vi)
            inv_twist[row, 2 * part] = rr
            inv_twist[row, 2 * part + 1] = ri
        ur, ui = cosine_sine(k_ids * shift, length)
        ramp[row, 0] = ur
        ramp[row, 1] = -ui
        return carry

    twist_load.wait()
    lax.fori_loop(0, row_count, prepare, 0)

    one_load.wait()
    two_load.wait()

    def lefts(blocks):
        highs, lows = [], []
        for re, im in blocks:
            high, low = split(jnp.concatenate([re, im], 1))
            highs.append(high)
            lows.append(low)
        high, low = jnp.concatenate(highs, 0), jnp.concatenate(lows, 0)
        return jnp.concatenate([high, high, low], 1)

    chunks = outer // CHUNK

    def forward_rows(step, picks):
        rows = [recv[step, :, :, i].reshape(2 * outer, 2 * half) for i in picks]
        rights = []
        for side in range(2):
            lanes = slice(side * half, (side + 1) * half)
            right = jnp.concatenate([r[:, lanes] for r in rows], 1)
            rights.append(jnp.concatenate([right, right], 0))
        for chunk in range(chunks):
            ids = slice(chunk * CHUNK, (chunk + 1) * CHUNK)
            even, odd = [
                dot(one_ref[side, 2 * chunk * CHUNK : 2 * (chunk + 1) * CHUNK], rights[side])
                for side in range(2)
            ]
            blocks = []
            for e, value in enumerate((even + odd, even - odd)):
                tr, ti = twist_ref[2 * e, ids], twist_ref[2 * e + 1, ids]
                for k in range(len(picks)):
                    lanes = slice(k * half, (k + 1) * half)
                    blocks.append(cmul(value[:CHUNK, lanes], value[CHUNK:, lanes], tr, ti))
            got = dot(lefts(blocks), two_ref[0])
            for e in range(2):
                for k, i in enumerate(picks):
                    base = (e * len(picks) + k) * CHUNK
                    spec[step, chunk, e, i] = got[base : base + CHUNK]

    def forward(step, carry):
        arrived = recv.at[step, pl.ds(0, len(peers))]
        pltpu.make_async_copy(arrived, arrived, recv_sem.at[step]).wait()
        forward_rows(step, range(PAIR))
        return carry

    def inverse_rows(step, picks):
        count = len(picks)
        for chunk in range(outer // BACK):
            ids = slice(chunk * BACK, (chunk + 1) * BACK)
            first = chunk * BACK % CHUNK
            blocks = []
            for e in range(2):
                lanes = slice(e * half, (e + 1) * half)
                for i in picks:
                    row = step * PAIR + i
                    picked = filt_all[slabs_ref[row], :, e, ids].astype(f32)
                    ur, ui = ramp[row, 0][:1, lanes], ramp[row, 1][:1, lanes]
                    gr, gi = cmul(picked[0], picked[1], ur, ui)
                    z = spec[step, chunk * BACK // CHUNK, e, i, first : first + BACK]
                    blocks.append(cmul(z[:, :half], z[:, half:], gr, gi))
            back = dot(lefts(blocks), two_ref[1])
            for k, i in enumerate(picks):
                row = step * PAIR + i
                got = []
                for e in range(2):
                    base = (e * count + k) * BACK
                    u = back[base : base + BACK]
                    got.append(
                        cmul(
                            u[:, :half], u[:, half:],
                            inv_twist[row, 2 * e, ids], inv_twist[row, 2 * e + 1, ids],
                        )
                    )
                lanes = slice(k * half, (k + 1) * half)
                for part in range(2):
                    to = slice(part * outer + chunk * BACK, part * outer + (chunk + 1) * BACK)
                    for side, value in enumerate((got[0][part] + got[1][part], got[0][part] - got[1][part])):
                        high, low = split(value)
                        middle[side, 0, to, lanes] = high
                        middle[side, 1, to, lanes] = low

    def image_rows(step, picks):
        rows = outer // strips
        width = len(picks) * half
        for side in range(2):
            high, low = middle[side, 0, :, :width], middle[side, 1, :, :width]
            res = dot(last_ref[side], jnp.concatenate([high, high, low], 0))
            for k, i in enumerate(picks):
                place = lax.rem(step, 8 // PAIR) * PAIR + i + 8 * side
                for part in range(2):
                    out_ref[part, step // (8 // PAIR), pl.ds(place, rows, stride=16), :] = res[
                        part * rows : (part + 1) * rows, k * half : (k + 1) * half
                    ]

    def inverse(step, carry):
        inverse_rows(step, range(PAIR))
        return lax.fori_loop(step, step + 1, image, carry)

    def image(step, carry):
        image_rows(step, range(PAIR))
        return carry

    def both(step, carry):
        forward(step, 0)
        inverse(step, 0)
        return carry

    early = pairs // 2
    def pass_on(j):
        origin = jnp.where(blk + j < blks, blk + j, blks - 1 - j)
        dz = lax.rem(blk - origin + blks, blks)
        filter_copy(dz).wait_recv()
        relay_copy(dz).start()

    lax.fori_loop(0, early - 1, forward, 0)
    for j in range(1, blks - 1):
        pass_on(j)
    lax.fori_loop(early - 1, early, forward, 0)
    pass_on(blks - 1)
    others = filt_all.at[pl.ds(0, (blks - 1) * slab_local), 0]
    pltpu.make_async_copy(others, others, grecv.at[0]).wait()
    last_load.wait()
    lax.fori_loop(0, early, inverse, 0)
    lax.fori_loop(early, pairs, both, 0)

    sent = recv.at[:, pl.ds(0, len(peers))]
    pltpu.make_async_copy(sent, sent, send_sem.at[0]).wait()
    pltpu.make_async_copy(others, others, fsend.at[0]).wait()
    pltpu.make_async_copy(others, others, gsend.at[0]).wait()


def per_device(turns, blks, strips, echoes, filters, slab_index, shifts):
    sources = turns * strips
    length = filters.shape[2]
    half = LANES
    outer = length // (2 * half)
    local = outer // sources
    row_count = slab_index.shape[0]
    slab_local = filters.shape[1]
    pairs = row_count // PAIR
    shaped = echoes.reshape(2, -1, 8, 2 * local, half).transpose(0, 1, 3, 2, 4)
    response = filters.reshape(2, slab_local, 2 * outer, half).transpose(0, 2, 1, 3)
    response = response.reshape(2, -1, half)
    tables = [jnp.asarray(t) for t in make_tables(length, sources, strips)]
    hbm, smem = pl.BlockSpec(memory_space=pltpu.HBM), pl.BlockSpec(memory_space=pltpu.SMEM)
    rows = outer // strips
    image = pl.pallas_call(
        functools.partial(body, turns, blks, strips, length),
        out_shape=pltpu.VMEM((2, row_count // 8, rows * 16, half), f32),
        in_specs=[smem, smem] + [hbm] * 6,
        out_specs=pl.BlockSpec(memory_space=pltpu.VMEM),
        scratch_shapes=[
            pltpu.VMEM((pairs, sources, 2, PAIR, local, 2 * half), bf16),
            pltpu.VMEM((slab_local * blks, 2, 2, outer, half), bf16),
            pltpu.VMEM((row_count, 4, outer, half), f32),
            pltpu.VMEM((row_count, 2, 8, 2 * half), f32),
            pltpu.VMEM((pairs, outer // CHUNK, 2, PAIR, CHUNK, 2 * half), f32),
            pltpu.VMEM((2, 2, 2 * outer, 2 * half), bf16),
            pltpu.VMEM(tables[0].shape, bf16),
            pltpu.VMEM(tables[1].shape, bf16),
            pltpu.VMEM(tables[2].shape, f32),
            pltpu.VMEM(tables[3].shape[1:], bf16),
            pltpu.VMEM(shaped.shape, bf16),
            pltpu.VMEM(response.shape, bf16),
            pltpu.VMEM((turns, 2, 16 * local, half), f32),
            pltpu.VMEM((turns, pairs, 2, PAIR, local, 2 * half), bf16),
            pltpu.SemaphoreType.DMA((1,)),
            pltpu.SemaphoreType.DMA((pairs,)),
            pltpu.SemaphoreType.DMA((1,)),
            pltpu.SemaphoreType.DMA((blks,)),
            pltpu.SemaphoreType.DMA((1,)),
            pltpu.SemaphoreType.DMA((1,)),
            pltpu.SemaphoreType.DMA((6 + row_count // 8,)),
        ],
        compiler_params=pltpu.CompilerParams(
            collective_id=0, has_side_effects=True, vmem_limit_bytes=56 * 1024 * 1024
        ),
    )(shifts, slab_index, shaped, response, *tables)
    image = image.reshape(2, row_count // 8, rows * 2, 8, half).transpose(0, 1, 3, 2, 4)
    return image.reshape(2, row_count, rows * 2 * half)


def solution(mesh):
    in_specs = (
        P(None, "blk", ("turn", "strip")),
        P(None, "blk", None),
        P(("blk", "turn")),
        P(("blk", "turn")),
    )
    out_specs = P(None, ("blk", "turn"), "strip")
    local = functools.partial(
        per_device, mesh.shape["turn"], mesh.shape["blk"], mesh.shape["strip"]
    )
    return jax.shard_map(local, mesh=mesh, in_specs=in_specs, out_specs=out_specs, check_vma=False)
```

```python
import functools
import math

import jax
import jax.numpy as jnp
import numpy as np
from jax import lax
from jax.experimental import pallas as pl
from jax.experimental.pallas import tpu as pltpu
from jax.sharding import PartitionSpec as P

LANES = 128
PAIR = 2
CHUNK = 64
BACK = 32
MESH = pl.DeviceIdType.MESH
f32, bf16 = jnp.float32, jnp.bfloat16


def split_np(table):
    high = table.astype(jnp.bfloat16)
    low = (table - high.astype(np.float64)).astype(jnp.bfloat16)
    return high, low


def make_tables(length, sources, strips):
    half = LANES
    outer = length // (2 * half)
    local = outer // sources
    a_ids, c_ids = np.arange(outer), np.arange(outer)
    b_ids = np.arange(half)
    tau = np.exp(-2j * np.pi * half * c_ids / length)
    first = np.exp(-2j * np.pi * ((c_ids[:, None] * a_ids[None, :]) % outer) / outer)
    stage_one = []
    for mat in (first, tau[:, None] * first):
        grouped = mat.reshape(outer, sources, 1, local)
        top = np.concatenate([grouped.real, -grouped.imag], 2).reshape(-1, CHUNK, 2 * outer)
        bottom = np.concatenate([grouped.imag, grouped.real], 2).reshape(-1, CHUNK, 2 * outer)
        whole = np.concatenate([top, bottom], 1).reshape(2 * outer, 2 * outer)
        stage_one.append(np.concatenate(split_np(whole), 1))
    stage_one = np.stack(stage_one)
    base = np.exp(-2j * np.pi * ((b_ids[:, None] * b_ids[None, :]) % half) / half)

    def right(mat):
        whole = np.concatenate(
            [np.concatenate([mat.real, mat.imag], 1), np.concatenate([-mat.imag, mat.real], 1)], 0
        )
        high, low = split_np(whole)
        return np.concatenate([high, low, high], 0)

    stage_two = np.stack([right(base), right(base.conj())])
    twist = np.exp(-2j * np.pi * ((c_ids[:, None] * b_ids[None, :]) % length) / length)
    omega = np.exp(-2j * np.pi * b_ids / (2 * half))
    turned = twist * omega[None, :]
    twists = np.stack([twist.real, twist.imag, turned.real, turned.imag]).astype(np.float32)
    rows = outer // strips
    last = []
    for strip in range(strips):
        picked = np.arange(strip * rows, (strip + 1) * rows)
        back = np.exp(2j * np.pi * ((picked[:, None] * c_ids[None, :]) % outer) / outer) / length
        per_half = []
        for mat in (back, back * tau.conj()[None, :]):
            whole = np.concatenate(
                [np.concatenate([mat.real, -mat.imag], 1), np.concatenate([mat.imag, mat.real], 1)], 0
            )
            high, low = split_np(whole)
            per_half.append(np.concatenate([high, low, high], 1))
        last.append(np.stack(per_half))
    return stage_one, stage_two, twists, np.stack(last)


def cosine_sine(phase, length):
    quarter = length // 4
    wrapped = phase & (length - 1)
    quadrant = (wrapped + quarter // 2) // quarter if quarter & (quarter - 1) else (
        wrapped + quarter // 2
    ) >> (quarter.bit_length() - 1)
    angle = (wrapped - quadrant * quarter).astype(f32) * (2.0 * math.pi / length)
    square = angle * angle
    sine = angle * (
        1.0 + square * (-1.0 / 6 + square * (1.0 / 120 + square * (-1.0 / 5040 + square * (1.0 / 362880))))
    )
    cosine = 1.0 + square * (
        -0.5
        + square * (1.0 / 24 + square * (-1.0 / 720 + square * (1.0 / 40320 - square * (1.0 / 3628800))))
    )
    odd = (quadrant & 1) == 1
    out_cos = jnp.where(odd, sine, cosine)
    out_sin = jnp.where(odd, cosine, sine)
    quad = quadrant & 3
    out_cos = jnp.where((quad == 1) | (quad == 2), -out_cos, out_cos)
    out_sin = jnp.where(quad >= 2, -out_sin, out_sin)
    return out_cos, out_sin


def cmul(ar, ai, br, bi):
    return ar * br - ai * bi, ar * bi + ai * br


def split(values):
    high = values.astype(bf16)
    return high, (values - high.astype(f32)).astype(bf16)


def dot(left, right):
    return jnp.dot(left, right, preferred_element_type=f32)


def body(
    turns, blks, strips, length,
    shifts_ref, slabs_ref, ech_ref, filt_ref, one_hbm, two_hbm, twist_hbm, last_hbm,
    out_ref,
    recv, filt_all, inv_twist, ramp, spec, middle, one_ref, two_ref, twist_ref, last_ref, ech_raw, filt_raw, staged, outbox,
    send_sem, recv_sem, fsend, frecv, gsend, grecv, load_sem,
):
    turn, blk, strip = lax.axis_index("turn"), lax.axis_index("blk"), lax.axis_index("strip")
    pairs = recv.shape[0]
    row_count = pairs * PAIR
    slab_local = filt_ref.shape[1] * LANES // length
    core = lax.rem(turn, 2)
    partner = turn + 1 - 2 * core
    peers = [
        (dt, ds) for dt in range(turns) for ds in range(strips) if (dt, ds) != (0, 0)
    ]
    peers.sort(key=lambda p: (p[1] == 0, p[0] % 2, p[0] < 2, p))

    def peer(dt, ds):
        to = lax.rem(turn - core + (dt // 2) * 2, turns) + lax.rem(core + dt, 2)
        return (to, blk, lax.rem(strip + ds, strips))

    me = turn * strips + strip
    twist_load = pltpu.make_async_copy(twist_hbm, twist_ref, load_sem.at[0])
    one_load = pltpu.make_async_copy(one_hbm, one_ref, load_sem.at[1])
    two_load = pltpu.make_async_copy(two_hbm, two_ref, load_sem.at[2])
    last_load = pltpu.make_async_copy(last_hbm.at[strip], last_ref, load_sem.at[3])
    filter_load = pltpu.make_async_copy(filt_ref, filt_raw, load_sem.at[5])
    groups = row_count // 8
    per_group = 8 // PAIR

    def load_group(group):
        for to in range(turns):
            block = pl.ds(to * groups + group, 1)
            pltpu.make_async_copy(
                ech_ref.at[:, block], ech_raw.at[:, block], load_sem.at[6 + group]
            ).start()

    load_group(0)
    filter_load.start()

    barrier = pltpu.get_barrier_semaphore()
    for dt, ds in peers:
        pl.semaphore_signal(barrier, inc=1, device_id=peer(dt, ds), device_id_type=MESH)
    def signal_blk(to):
        pl.semaphore_signal(barrier, inc=1, device_id=(turn, to, strip), device_id_type=MESH)

    def echo_copy(step, dt, ds):
        to = peer(dt, ds)
        return pltpu.make_async_remote_copy(
            src_ref=outbox.at[to[0], step],
            dst_ref=recv.at[step, me],
            send_sem=send_sem.at[0],
            recv_sem=recv_sem.at[step],
            device_id=to,
            device_id_type=MESH,
        )

    def filter_copy(dz):
        return pltpu.make_async_remote_copy(
            src_ref=filt_all.at[pl.ds(blk * slab_local, slab_local), core],
            dst_ref=filt_all.at[pl.ds(blk * slab_local, slab_local), core],
            send_sem=fsend.at[0],
            recv_sem=frecv.at[dz],
            device_id=(turn, lax.rem(blk + dz, blks), strip),
            device_id_type=MESH,
        )

    def relay_copy(dz):
        origin = lax.rem(blk + blks - dz, blks)
        place = filt_all.at[pl.ds(origin * slab_local, slab_local), core]
        return pltpu.make_async_remote_copy(
            src_ref=place,
            dst_ref=place,
            send_sem=gsend.at[0],
            recv_sem=grecv.at[0],
            device_id=(partner, blk, strip),
            device_id_type=MESH,
        )

    half = LANES
    outer = length // (2 * half)
    local = ech_raw.shape[2] // 2
    def stage(group):
        whole = ech_raw.at[:, pl.ds(0, turns)]
        pltpu.make_async_copy(whole, whole, load_sem.at[6 + group]).wait()

        def fill(to, carry):
            for part in range(2):
                values = ech_raw[part, to * groups + group].astype(f32)
                staged[to, part] = values.reshape(2 * local * 8, half)
            return carry

        lax.fori_loop(0, turns, fill, 0)

    def pick(step):
        first = lax.rem(step, per_group) * PAIR

        def fill(to, carry):
            for part in range(2):
                for row in range(PAIR):
                    for side in range(2):
                        value = staged[to, part, pl.ds(first + side * 8 + row, local, stride=16), :]
                        outbox[
                            to, step, part, row, :, side * half : (side + 1) * half
                        ] = value.astype(bf16)
            return carry

        lax.fori_loop(0, turns, fill, 0)

    def send(step):
        for dt, ds in peers:
            echo_copy(step, dt, ds).start()
        recv[step, me] = outbox[turn, step]

    def pick_send(step, carry):
        pick(step)
        send(step)
        return carry

    stage(0)
    for group in range(1, groups):
        load_group(group)
    pick(0)
    pl.semaphore_wait(barrier, len(peers) + jnp.where(blk > 0, 1, 0))
    send(0)

    @pl.when(blk < blks - 1)
    def _():
        signal_blk(blk + 1)

    @pl.when(blk == blks - 1)
    def _():
        signal_blk(blk - 1)

    filter_load.wait()
    bins = filt_raw.shape[1]
    bin_ids = lax.broadcasted_iota(jnp.int32, (bins, half), 0)
    d_ids = lax.broadcasted_iota(jnp.int32, (bins, half), 1)
    for s in range(slab_local):
        for e in range(2):
            picker = (bin_ids == (d_ids * 2 + e) * slab_local + s).astype(f32).astype(bf16)
            for part in range(2):
                got = lax.dot_general(
                    filt_raw[part], picker, (((0,), (0,)), ((), ())), preferred_element_type=f32
                )
                filt_all[blk * slab_local + s, part, e] = got.astype(bf16)
    for dz in range(1, blks):

        @pl.when(blk + dz >= blks)
        def _(dz=dz):
            filter_copy(dz).start()

    lax.fori_loop(1, per_group, pick_send, 0)
    twist_load.start()
    one_load.start()
    two_load.start()
    last_load.start()

    @pl.when(blk < blks - 1)
    def _():
        pl.semaphore_wait(barrier, 1)

        @pl.when(blk > 0)
        def _():
            signal_blk(blk - 1)

        for dz in range(1, blks):

            @pl.when(blk + dz < blks)
            def _(dz=dz):
                filter_copy(dz).start()

    for group in range(1, groups):
        stage(group)
        lax.fori_loop(group * per_group, (group + 1) * per_group, pick_send, 0)
    c_ids = lax.broadcasted_iota(jnp.int32, (outer, half), 0)
    lane_ids = lax.broadcasted_iota(jnp.int32, (8, 2 * half), 1)
    k_ids = jnp.where(lane_ids >= half, (lane_ids - half) * (2 * outer) + outer, lane_ids * (2 * outer))

    def prepare(row, carry):
        shift = shifts_ref[row]
        vr, vi = cosine_sine(c_ids * shift, length)
        vi = -vi
        for part in range(2):
            tr, ti = twist_ref[2 * part], -twist_ref[2 * part + 1]
            rr, ri = cmul(tr, ti, vr, vi)
            inv_twist[row, 2 * part] = rr
            inv_twist[row, 2 * part + 1] = ri
        ur, ui = cosine_sine(k_ids * shift, length)
        ramp[row, 0] = ur
        ramp[row, 1] = -ui
        return carry

    twist_load.wait()
    lax.fori_loop(0, row_count, prepare, 0)

    one_load.wait()
    two_load.wait()

    def lefts(blocks):
        highs, lows = [], []
        for re, im in blocks:
            high, low = split(jnp.concatenate([re, im], 1))
            highs.append(high)
            lows.append(low)
        high, low = jnp.concatenate(highs, 0), jnp.concatenate(lows, 0)
        return jnp.concatenate([high, high, low], 1)

    chunks = outer // CHUNK

    def forward_rows(step, picks):
        rows = [recv[step, :, :, i].reshape(2 * outer, 2 * half) for i in picks]
        rights = []
        for side in range(2):
            lanes = slice(side * half, (side + 1) * half)
            right = jnp.concatenate([r[:, lanes] for r in rows], 1)
            rights.append(jnp.concatenate([right, right], 0))
        for chunk in range(chunks):
            ids = slice(chunk * CHUNK, (chunk + 1) * CHUNK)
            even, odd = [
                dot(one_ref[side, 2 * chunk * CHUNK : 2 * (chunk + 1) * CHUNK], rights[side])
                for side in range(2)
            ]
            blocks = []
            for e, value in enumerate((even + odd, even - odd)):
                tr, ti = twist_ref[2 * e, ids], twist_ref[2 * e + 1, ids]
                for k in range(len(picks)):
                    lanes = slice(k * half, (k + 1) * half)
                    blocks.append(cmul(value[:CHUNK, lanes], value[CHUNK:, lanes], tr, ti))
            got = dot(lefts(blocks), two_ref[0])
            for e in range(2):
                for k, i in enumerate(picks):
                    base = (e * len(picks) + k) * CHUNK
                    spec[step, chunk, e, i] = got[base : base + CHUNK]

    def forward(step, carry):
        arrived = recv.at[step, pl.ds(0, len(peers))]
        pltpu.make_async_copy(arrived, arrived, recv_sem.at[step]).wait()
        forward_rows(step, range(PAIR))
        return carry

    def inverse_rows(step, picks):
        count = len(picks)
        for chunk in range(outer // BACK):
            ids = slice(chunk * BACK, (chunk + 1) * BACK)
            first = chunk * BACK % CHUNK
            blocks = []
            for e in range(2):
                lanes = slice(e * half, (e + 1) * half)
                for i in picks:
                    row = step * PAIR + i
                    picked = filt_all[slabs_ref[row], :, e, ids].astype(f32)
                    ur, ui = ramp[row, 0][:1, lanes], ramp[row, 1][:1, lanes]
                    gr, gi = cmul(picked[0], picked[1], ur, ui)
                    z = spec[step, chunk * BACK // CHUNK, e, i, first : first + BACK]
                    blocks.append(cmul(z[:, :half], z[:, half:], gr, gi))
            back = dot(lefts(blocks), two_ref[1])
            for k, i in enumerate(picks):
                row = step * PAIR + i
                got = []
                for e in range(2):
                    base = (e * count + k) * BACK
                    u = back[base : base + BACK]
                    got.append(
                        cmul(
                            u[:, :half], u[:, half:],
                            inv_twist[row, 2 * e, ids], inv_twist[row, 2 * e + 1, ids],
                        )
                    )
                lanes = slice(k * half, (k + 1) * half)
                for part in range(2):
                    to = slice(part * outer + chunk * BACK, part * outer + (chunk + 1) * BACK)
                    for side, value in enumerate((got[0][part] + got[1][part], got[0][part] - got[1][part])):
                        high, low = split(value)
                        middle[side, 0, to, lanes] = high
                        middle[side, 1, to, lanes] = low

    def image_rows(step, picks):
        rows = outer // strips
        width = len(picks) * half
        for side in range(2):
            high, low = middle[side, 0, :, :width], middle[side, 1, :, :width]
            res = dot(last_ref[side], jnp.concatenate([high, high, low], 0))
            for k, i in enumerate(picks):
                place = lax.rem(step, 8 // PAIR) * PAIR + i + 8 * side
                for part in range(2):
                    out_ref[part, step // (8 // PAIR), pl.ds(place, rows, stride=16), :] = res[
                        part * rows : (part + 1) * rows, k * half : (k + 1) * half
                    ]

    def inverse(step, carry):
        inverse_rows(step, range(PAIR))
        image_rows(step, range(PAIR))
        return carry

    def both(step, carry):
        forward(step, 0)
        inverse(step, 0)
        return carry

    early = pairs // 2
    def pass_on(j):
        origin = jnp.where(blk + j < blks, blk + j, blks - 1 - j)
        dz = lax.rem(blk - origin + blks, blks)
        filter_copy(dz).wait_recv()
        relay_copy(dz).start()

    lax.fori_loop(0, early - 1, forward, 0)
    for j in range(1, blks - 1):
        pass_on(j)
    lax.fori_loop(early - 1, early, forward, 0)
    pass_on(blks - 1)
    others = filt_all.at[pl.ds(0, (blks - 1) * slab_local), 0]
    pltpu.make_async_copy(others, others, grecv.at[0]).wait()
    last_load.wait()
    lax.fori_loop(0, early, inverse, 0)
    lax.fori_loop(early, pairs, both, 0)

    sent = recv.at[:, pl.ds(0, len(peers))]
    pltpu.make_async_copy(sent, sent, send_sem.at[0]).wait()
    pltpu.make_async_copy(others, others, fsend.at[0]).wait()
    pltpu.make_async_copy(others, others, gsend.at[0]).wait()


def per_device(turns, blks, strips, echoes, filters, slab_index, shifts):
    sources = turns * strips
    length = filters.shape[2]
    half = LANES
    outer = length // (2 * half)
    local = outer // sources
    row_count = slab_index.shape[0]
    slab_local = filters.shape[1]
    pairs = row_count // PAIR
    shaped = echoes.reshape(2, -1, 8, 2 * local, half).transpose(0, 1, 3, 2, 4)
    response = filters.reshape(2, slab_local, 2 * outer, half).transpose(0, 2, 1, 3)
    response = response.reshape(2, -1, half)
    tables = [jnp.asarray(t) for t in make_tables(length, sources, strips)]
    hbm, smem = pl.BlockSpec(memory_space=pltpu.HBM), pl.BlockSpec(memory_space=pltpu.SMEM)
    rows = outer // strips
    image = pl.pallas_call(
        functools.partial(body, turns, blks, strips, length),
        out_shape=pltpu.VMEM((2, row_count // 8, rows * 16, half), f32),
        in_specs=[smem, smem] + [hbm] * 6,
        out_specs=pl.BlockSpec(memory_space=pltpu.VMEM),
        scratch_shapes=[
            pltpu.VMEM((pairs, sources, 2, PAIR, local, 2 * half), bf16),
            pltpu.VMEM((slab_local * blks, 2, 2, outer, half), bf16),
            pltpu.VMEM((row_count, 4, outer, half), f32),
            pltpu.VMEM((row_count, 2, 8, 2 * half), f32),
            pltpu.VMEM((pairs, outer // CHUNK, 2, PAIR, CHUNK, 2 * half), f32),
            pltpu.VMEM((2, 2, 2 * outer, 2 * half), bf16),
            pltpu.VMEM(tables[0].shape, bf16),
            pltpu.VMEM(tables[1].shape, bf16),
            pltpu.VMEM(tables[2].shape, f32),
            pltpu.VMEM(tables[3].shape[1:], bf16),
            pltpu.VMEM(shaped.shape, bf16),
            pltpu.VMEM(response.shape, bf16),
            pltpu.VMEM((turns, 2, 16 * local, half), f32),
            pltpu.VMEM((turns, pairs, 2, PAIR, local, 2 * half), bf16),
            pltpu.SemaphoreType.DMA((1,)),
            pltpu.SemaphoreType.DMA((pairs,)),
            pltpu.SemaphoreType.DMA((1,)),
            pltpu.SemaphoreType.DMA((blks,)),
            pltpu.SemaphoreType.DMA((1,)),
            pltpu.SemaphoreType.DMA((1,)),
            pltpu.SemaphoreType.DMA((6 + row_count // 8,)),
        ],
        compiler_params=pltpu.CompilerParams(
            collective_id=0, has_side_effects=True, vmem_limit_bytes=56 * 1024 * 1024
        ),
    )(shifts, slab_index, shaped, response, *tables)
    image = image.reshape(2, row_count // 8, rows * 2, 8, half).transpose(0, 1, 3, 2, 4)
    return image.reshape(2, row_count, rows * 2 * half)


def solution(mesh):
    in_specs = (
        P(None, "blk", ("turn", "strip")),
        P(None, "blk", None),
        P(("blk", "turn")),
        P(("blk", "turn")),
    )
    out_specs = P(None, ("blk", "turn"), "strip")
    local = functools.partial(
        per_device, mesh.shape["turn"], mesh.shape["blk"], mesh.shape["strip"]
    )
    return jax.shard_map(local, mesh=mesh, in_specs=in_specs, out_specs=out_specs, check_vma=False)
```
